128 devices in a mesh: dp: 64 (over x, y, z_lo, core), section: 2 (over z_hi).
Axes of the slice: x: 4, y: 4, z: 4 (z_hi: 2, z_lo: 2; z = z_hi * 2 + z_lo), core: 2. Of those that a mesh axis runs over, the one named last changes fastest.
Arguments:
- samples: bfloat16 [512, 512], P('dp'), may hold values from -16 to 16
- targets: bfloat16 [512, 512], P('dp'), may hold values from -16 to 16
- jacobian_targets: bfloat16 [512, 128, 512], P('dp'), may hold values from -0.1796875 to 0.1796875
- directions: int32 [512, 128], P('dp'), may hold values from 0 to 511
- plan: int32 [64, 8], P('dp'), may hold values from 0 to 7, each once within a row
- weights: bfloat16 [2, 512, 8192], P('section'), may hold values from -1 to 1
Outputs:
- gradients: float32 [2, 512, 8192], P('section', 'dp')
The draws below stay inside these ranges and needn't reach their ends.
Inputs may be any that keep to these rules, and one draw needn't show every extreme that they name: `plan`: each row is a permutation of 0 to 7.
All inputs are finite; a program needn't handle non-finite values.
Results may differ from the reference program's by a relative error of at most 0.0034.
Values may be sent and summed in bfloat16 or wider, within the bound.
No kernel may reach another device: no remote copies, remote signals or barrier semaphores. Data moves between devices by JAX's collectives and lax.ppermute only.
A program may use at most 128 MiB of HBM per device.

```python
import jax
import jax.numpy as jnp
from jax import lax

REDUCED = 512
WIDTH = 8192
TANGENTS = 128
MICRO = 4
BATCH = 1
POOL = 8
SAMPLES = 512
N_DP = 64


def draw_weights(key, part):
    scales = jnp.array([REDUCED ** (-0.5), WIDTH ** (-0.5)], jnp.float32)[:, None, None]
    base = jnp.clip(jax.random.normal(key, (2, REDUCED, WIDTH), jnp.float32), -4.0, 4.0)
    return (base * scales).astype(jnp.bfloat16)


def place_ends(values, own_key, smallest, largest):
    extent = values.shape
    index_at = [jax.random.randint(jax.random.fold_in(own_key, axis), (), 0, extent[axis]) for axis in range(len(extent))]
    values = values.at[tuple(index_at)].set(smallest)
    longest = extent.index(max(extent))
    index_at[longest] = (index_at[longest] + 1) % extent[longest]
    return values.at[tuple(index_at)].set(largest)


def raised(values, stream_key, source, target, parts, factor):
    owner, partner = [(jnp.arange(values.shape[dim]) // (values.shape[dim] // parts)).reshape([-1 if axis == dim else 1 for axis in range(values.ndim)]) for dim in (source, target)]
    chosen = jax.random.permutation(stream_key, parts)[partner]
    strong = (owner == chosen) | (owner == (partner + parts // 2) % parts)
    return jnp.where(strong, factor * values, values)


def levels(own_key, extent, split, low, largest):
    loudness = 1.0
    for axis_at, parts in split:
        heights = jax.random.uniform(jax.random.fold_in(jax.random.fold_in(own_key, 6), axis_at), (parts,), jnp.float32, low / len(split), largest / len(split))
        loudness = loudness * jnp.repeat(jnp.exp(heights), extent[axis_at] // parts).reshape((-1,) + (1,) * (len(extent) - 1 - axis_at))
    return loudness


def gaussian(stream_key, extent, spread, most, split=(), held_as=jnp.bfloat16):
    loudness = levels(stream_key, extent, split, -0.22, 0.18) if split else 1.0
    result = jax.random.normal(stream_key, extent, jnp.float32) * spread * loudness
    return jnp.minimum(jnp.maximum(result, -most), most).astype(held_as)


def gaussian_with(stream_key, extent, scale, bound, pieces, heavy, kind=jnp.bfloat16):
    entries = scale * jax.random.normal(stream_key, extent, jnp.float32)
    if pieces:
        entries = entries * levels(stream_key, extent, pieces, -0.22, 0.18)
    return jnp.clip(raised(entries, jax.random.fold_in(stream_key, 3), *heavy), -bound, bound).astype(kind)


def setup_inputs(seed: int = 0) -> dict:
    arg_keys = jax.random.split(jax.random.key(seed), 7)
    samples = gaussian_with(arg_keys[0], (SAMPLES, REDUCED), 1.0, 16.0, ((0, 64),), (0, 1, 64, 4.0))
    targets = gaussian_with(arg_keys[1], (SAMPLES, REDUCED), 1.0, 16.0, ((0, 64),), (0, 1, 64, 4.0))
    jacobian_targets = gaussian(arg_keys[2], (SAMPLES, TANGENTS, REDUCED), 0.03, 0.1796875, ((0, 64),))
    directions = place_ends(jax.random.randint(arg_keys[3], (SAMPLES, TANGENTS), 0, REDUCED), jax.random.fold_in(arg_keys[3], 1), 0, REDUCED - 1).astype(jnp.int32)
    plan = jax.vmap(lambda own: jax.random.permutation(own, POOL))(jax.random.split(arg_keys[4], N_DP)).reshape((N_DP, POOL)).astype(jnp.int32)
    weights = draw_weights(jax.random.fold_in(arg_keys[6], 71), 0)
    return dict(samples=samples, targets=targets, jacobian_targets=jacobian_targets, directions=directions, plan=plan, weights=weights)


jacobian_weight = 32.0


def contract_rows(left, right):
    return lax.dot_general(left, right, (((0,), (0,)), ((), ())), preferred_element_type=jnp.float32)


def against_rows(left, right):
    return lax.dot_general(left, right, (((1,), (1,)), ((), ())), preferred_element_type=jnp.float32)


def encoder_parts(inputs, chosen_dirs, w_first):
    linear = jnp.dot(inputs, w_first, preferred_element_type=jnp.float32)
    squash = jax.nn.sigmoid(linear)
    first_slope = squash * (1.0 + linear * (1.0 - squash))
    second_slope = squash * (1.0 - squash) * (2.0 + linear * (1.0 - 2.0 * squash))
    picked = jnp.take(w_first, chosen_dirs, axis=0)
    return linear, squash, first_slope, second_slope, picked


def encoder_forward(encoded):
    linear, squash, first_slope, second_slope, picked = encoded
    hidden = (linear * squash).astype(jnp.bfloat16)
    tangent = (first_slope[:, None, :] * picked.astype(jnp.float32)).astype(jnp.bfloat16)
    return hidden, tangent


def decoder(hidden, tangent, w_last, target_rows, jacobian_rows):
    columns = hidden.shape[1]
    flattened = tangent.reshape(-1, columns)
    output = against_rows(hidden, w_last)
    jacobian = against_rows(flattened, w_last)
    misfit = (output - target_rows.astype(jnp.float32)).astype(jnp.bfloat16)
    jac_misfit = (jacobian_weight * (jacobian - jacobian_rows.reshape(jacobian.shape).astype(jnp.float32))).astype(jnp.bfloat16)
    grad_last = contract_rows(misfit, hidden) + contract_rows(jac_misfit, flattened)
    cotangent = jnp.dot(misfit, w_last, preferred_element_type=jnp.float32).astype(jnp.bfloat16)
    cotangent_tangent = jnp.dot(jac_misfit, w_last, preferred_element_type=jnp.float32).astype(jnp.bfloat16)
    return grad_last, cotangent, cotangent_tangent.reshape(tangent.shape)


def encoder_backward(inputs, chosen_dirs, encoded, cotangent, cotangent_tangent, reduced):
    linear, squash, first_slope, second_slope, picked = encoded
    projected = jnp.sum(cotangent_tangent.astype(jnp.float32) * picked.astype(jnp.float32), axis=1)
    grad_pre = (cotangent.astype(jnp.float32) * first_slope + second_slope * projected).astype(jnp.bfloat16)
    grad_picked = (cotangent_tangent.astype(jnp.float32) * first_slope[:, None, :]).astype(jnp.bfloat16)
    columns = grad_pre.shape[1]
    onehot = (chosen_dirs.reshape(-1)[:, None] == jnp.arange(reduced, dtype=jnp.int32)[None, :]).astype(jnp.bfloat16)
    return contract_rows(inputs, grad_pre) + contract_rows(onehot, grad_picked.reshape(-1, columns))


def reference(samples, targets, jacobian_targets, directions, plan, weights):
    w_first = weights[0]
    w_last = weights[1]
    offsets = jnp.arange(N_DP, dtype=jnp.int32) * POOL
    picked_rows = (plan[:, :MICRO * BATCH].astype(jnp.int32) + offsets[:, None]).reshape(-1).astype(jnp.int32)

    def accumulate(carried, position):
        first_total, last_total = carried
        inputs = lax.dynamic_slice_in_dim(samples, position, 1, 0)
        chosen_dirs = lax.dynamic_slice_in_dim(directions, position, 1, 0)
        target_rows = lax.dynamic_slice_in_dim(targets, position, 1, 0)
        jacobian_rows = lax.dynamic_slice_in_dim(jacobian_targets, position, 1, 0)
        encoded = encoder_parts(inputs, chosen_dirs, w_first)
        hidden, tangent = encoder_forward(encoded)
        grad_last, cotangent, cotangent_tangent = decoder(hidden, tangent, w_last, target_rows, jacobian_rows)
        grad_first = encoder_backward(inputs, chosen_dirs, encoded, cotangent, cotangent_tangent, REDUCED)
        return (first_total + grad_first, last_total + grad_last), None

    cleared = jnp.zeros((REDUCED, WIDTH), jnp.float32)
    totals, unused = lax.scan(accumulate, (cleared, cleared), picked_rows)
    return jnp.stack([totals[0], totals[1]])
```

```python
import jax
import jax.numpy as jnp
from jax import lax
from jax.experimental import pallas as pl
from jax.experimental.pallas import tpu as pltpu
from jax.sharding import Mesh
from jax.sharding import PartitionSpec as P

AXES = ("x", "y", "zl", "core", "zh")
DP = ("x", "y", "zl", "core")
Z = ("zl", "zh")
MICRO = 4
REDUCED = 512
COLS = 1024
TANGENTS = 128
CHUNK = 2 * TANGENTS + 16
BLOCK = 256
jacobian_weight = 32.0
f32 = jnp.float32
bf16 = jnp.bfloat16


def z_index(z):
    return (z % 2) * 2 + z // 2


def z_shift(block, d):
    return lax.ppermute(block, Z, [(z_index(z), z_index((z + d) % 4)) for z in range(4)])


def ring_shift(block, axis, d):
    return lax.ppermute(block, axis, [(i, (i + d) % 4) for i in range(4)])


def core_swap(block):
    return lax.ppermute(block, "core", [(0, 1), (1, 0)])


def slopes(linear):
    squash = jax.nn.sigmoid(linear)
    first = squash * (1.0 + linear * (1.0 - squash))
    second = squash * (1.0 - squash) * (2.0 + linear * (1.0 - 2.0 * squash))
    return linear * squash, first, second


def per_row(top, first):
    return jnp.concatenate(
        [top[:TANGENTS] * first[0:1], top[TANGENTS : 2 * TANGENTS] * first[1:2]], axis=0
    )


def forward_kernel(place, rows, own, other, out, w_first, w_last):
    @pl.when(pl.program_id(0) == 0)
    def _():
        layer = place[1]
        w_first[...] = jnp.where(layer == 0, own[...], other[...])
        w_last[...] = jnp.where(layer == 0, other[...], own[...])

    picked = jnp.dot(rows[0], w_first[...], preferred_element_type=f32)
    hidden, first, _ = slopes(picked[2 * TANGENTS :])
    tangent = jnp.concatenate([per_row(picked, first), hidden], axis=0).astype(bf16)
    total = lax.dot_general(
        tangent, w_last[...], (((1,), (1,)), ((), ())), preferred_element_type=f32
    )
    out[0] = total.astype(out.dtype)


def forward(place, rows, weight, other, dtype):
    count = rows.shape[0]
    return pl.pallas_call(
        forward_kernel,
        grid_spec=pltpu.PrefetchScalarGridSpec(
            num_scalar_prefetch=1,
            grid=(count,),
            in_specs=[
                pl.BlockSpec((1, CHUNK, REDUCED), lambda i, place: (i, 0, 0)),
                pl.BlockSpec((REDUCED, COLS), lambda i, place: (0, place[0])),
                pl.BlockSpec((REDUCED, COLS), lambda i, place: (0, 0)),
            ],
            out_specs=pl.BlockSpec((1, CHUNK, REDUCED), lambda i, place: (i, 0, 0)),
            scratch_shapes=[
                pltpu.VMEM((REDUCED, COLS), bf16),
                pltpu.VMEM((REDUCED, COLS), bf16),
            ],
        ),
        out_shape=jax.ShapeDtypeStruct((count, CHUNK, REDUCED), dtype),
        compiler_params=pltpu.CompilerParams(dimension_semantics=("arbitrary",)),
        cost_estimate=pl.CostEstimate(
            flops=4 * count * CHUNK * REDUCED * COLS,
            bytes_accessed=4 * REDUCED * COLS,
            transcendentals=0,
        ),
    )(place, rows, weight, other)


def backward_kernel(place, rows, *refs):
    misfits = refs[:8]
    own, other, last_out, first_out, rows_t, misfit_t, tangents, cotangents = refs[8:]

    @pl.when(pl.program_id(0) == 0)
    def _():
        for k in range(8 * CHUNK // 128):
            rows_t[:, k * 128 : (k + 1) * 128] = rows[k * 128 : (k + 1) * 128, :].T
        whole = jnp.concatenate([m[...] for m in misfits], axis=0)
        for k in range(8 * CHUNK // 128):
            misfit_t[:, k * 128 : (k + 1) * 128] = whole[k * 128 : (k + 1) * 128, :].T

    layer = place[1]
    w_first = jnp.where(layer == 0, own[...], other[...])
    w_last = jnp.where(layer == 0, other[...], own[...])
    for c in range(8):
        span = pl.ds(c * CHUNK, CHUNK)
        picked = jnp.dot(rows[span, :], w_first, preferred_element_type=f32)
        hidden, first, second = slopes(picked[2 * TANGENTS :])
        tangents[span, :] = jnp.concatenate([per_row(picked, first), hidden], axis=0).astype(bf16)
        back = jnp.dot(misfits[c][...], w_last, preferred_element_type=f32)
        back = back.astype(bf16).astype(f32)
        joint = back[: 2 * TANGENTS] * picked[: 2 * TANGENTS]
        projected = jnp.concatenate(
            [
                jnp.sum(joint[:TANGENTS], axis=0, keepdims=True),
                jnp.sum(joint[TANGENTS:], axis=0, keepdims=True),
                jnp.zeros((14, BLOCK), f32),
            ],
            axis=0,
        )
        before = back[2 * TANGENTS :] * first + second * projected
        cotangents[span, :] = jnp.concatenate([per_row(back, first), before], axis=0).astype(bf16)
    last_out[...] = jnp.dot(misfit_t[...], tangents[...], preferred_element_type=f32).astype(bf16)
    first_out[...] = jnp.dot(rows_t[...], cotangents[...], preferred_element_type=f32).astype(bf16)


def backward(place, rows, misfits, weight, other):
    steps = COLS // BLOCK
    total = 8 * CHUNK
    return pl.pallas_call(
        backward_kernel,
        grid_spec=pltpu.PrefetchScalarGridSpec(
            num_scalar_prefetch=1,
            grid=(steps,),
            in_specs=[
                pl.BlockSpec((total, REDUCED), lambda j, place: (0, 0)),
                *[pl.BlockSpec((CHUNK, REDUCED), lambda j, place: (0, 0)) for _ in range(8)],
                pl.BlockSpec((REDUCED, BLOCK), lambda j, place: (0, place[0] * steps + j)),
                pl.BlockSpec((REDUCED, BLOCK), lambda j, place: (0, j)),
            ],
            out_specs=[
                pl.BlockSpec((REDUCED, BLOCK), lambda j, place: (0, j)),
                pl.BlockSpec((REDUCED, BLOCK), lambda j, place: (0, j)),
            ],
            scratch_shapes=[
                pltpu.VMEM((REDUCED, total), bf16),
                pltpu.VMEM((REDUCED, total), bf16),
                pltpu.VMEM((total, BLOCK), bf16),
                pltpu.VMEM((total, BLOCK), bf16),
            ],
        ),
        out_shape=[jax.ShapeDtypeStruct((REDUCED, COLS), bf16)] * 2,
        compiler_params=pltpu.CompilerParams(dimension_semantics=("arbitrary",)),
        cost_estimate=pl.CostEstimate(
            flops=8 * total * REDUCED * COLS, bytes_accessed=4 * REDUCED * COLS, transcendentals=0
        ),
    )(place, rows, *misfits, weight, other)


def ring_sum(chunks, at, axis):
    def piece(i):
        return lax.dynamic_index_in_dim(chunks, i % 4, 0, keepdims=False)

    got = [ring_shift(piece(at + d), axis, d) for d in (1, 3, 2)]
    total = piece(at).astype(f32)
    for g in got:
        total = total + g.astype(f32)
    return total


def shards(samples, targets, jacobian_targets, directions, plan, weights):
    at_x, at_y = lax.axis_index("x"), lax.axis_index("y")
    zl, core, zh = lax.axis_index("zl"), lax.axis_index("core"), lax.axis_index("zh")
    z = zh * 2 + zl
    weight = weights[0]
    mine = (zl * 2 + core) * 2 + zh
    theirs = ((1 - zl) * 2 + core) * 2 + (1 - zh)
    place = jnp.stack([mine, zh]).astype(jnp.int32)

    give = lax.dynamic_slice_in_dim(weight, theirs * COLS, COLS, 1)
    other = z_shift_partner(give)

    order = plan[0, :MICRO]
    inputs = jnp.take(samples, order, axis=0).astype(f32)
    chosen = jnp.take(directions, order, axis=0).astype(f32)
    small = lax.all_gather(jnp.concatenate([inputs, chosen], axis=1), ("zl", "core"))
    small = small.reshape(2, 2, 2, 2, REDUCED + TANGENTS).transpose(1, 2, 0, 3, 4)
    small = small.reshape(2, 4, 2, REDUCED + TANGENTS)
    small = jnp.where(core == 0, small, small[::-1])
    small = lax.dynamic_slice_in_dim(jnp.concatenate([small, small], axis=1), z, 4, 1)
    small = small.reshape(8, 2, REDUCED + TANGENTS)
    chosen = small[:, :, REDUCED:].reshape(8, 2 * TANGENTS).astype(jnp.int32)
    onehot = (chosen[:, :, None] == jnp.arange(REDUCED, dtype=jnp.int32)).astype(bf16)
    inputs = jnp.pad(small[:, :, :REDUCED].astype(bf16), ((0, 0), (0, 14), (0, 0)))
    rows = jnp.concatenate([onehot, inputs], axis=1)

    own_order = lax.dynamic_slice_in_dim(order, zh * 2, 2)
    target_rows = jnp.take(targets, own_order, axis=0).astype(f32)
    target_jac = jnp.take(jacobian_targets, own_order, axis=0).reshape(2 * TANGENTS, REDUCED)
    wanted = jnp.concatenate(
        [target_jac.astype(f32), jnp.pad(target_rows, ((0, 14), (0, 0)))], axis=0
    )

    sent = forward(place, rows[4:], weight, other, bf16)
    from_core = core_swap(sent)
    kept = forward(place, rows[:4], weight, other, f32)
    partial = kept + from_core.astype(f32)
    sending = partial[1:].astype(bf16)
    got = [z_shift(sending[d - 1], d) for d in (1, 3, 2)]
    total = partial[0]
    for g in got:
        total = total + g.astype(f32)
    scale = jnp.where(jnp.arange(CHUNK)[:, None] < 2 * TANGENTS, jacobian_weight, 1.0)
    misfit = (scale * (total - wanted)).astype(bf16)
    near = [misfit] + [z_shift(misfit, 4 - d) for d in (1, 2, 3)]
    far = [core_swap(m) for m in near]
    grad_last, grad_first = backward(
        place, rows.reshape(8 * CHUNK, REDUCED), near + far, weight, other
    )

    last = ring_sum(grad_last.reshape(4, 128, COLS), at_x, "x").astype(bf16)
    by_y = grad_first.reshape(4, 4, 32, COLS).transpose(1, 0, 2, 3)
    first = ring_sum(by_y, at_y, "y").astype(bf16)
    last = ring_sum(last.reshape(4, 32, COLS), at_y, "y")
    first = ring_sum(first, at_x, "x")

    both = jnp.stack([first.reshape(2, 2, 8, COLS), last.reshape(2, 2, 8, COLS)], axis=2)
    result = lax.all_to_all(
        both.reshape(8, 8, COLS), ("zl", "core", "zh"), split_axis=0, concat_axis=0, tiled=True
    )
    return result.transpose(1, 0, 2).reshape(1, 8, 8 * COLS)


def z_shift_partner(block):
    return lax.ppermute(block, Z, [(t, 3 - t) for t in range(4)])


def solution(mesh):
    torus = Mesh(mesh.devices.reshape(4, 4, 2, 2, 2), AXES)
    return jax.shard_map(
        shards,
        mesh=torus,
        in_specs=(
            P(DP, None),
            P(DP, None),
            P(DP, None, None),
            P(DP, None),
            P(DP, None),
            P("zh", None, None),
        ),
        out_specs=P("zh", DP, None),
        check_vma=False,
    )
```

```python
import jax
import jax.numpy as jnp
from jax import lax
from jax.experimental import pallas as pl
from jax.experimental.pallas import tpu as pltpu
from jax.sharding import Mesh
from jax.sharding import PartitionSpec as P

AXES = ("x", "y", "zl", "core", "zh")
DP = ("x", "y", "zl", "core")
Z = ("zl", "zh")
MICRO = 4
REDUCED = 512
COLS = 1024
HALF = COLS // 2
TANGENTS = 128
CHUNK = 2 * TANGENTS + 16
GROUP = 4 * CHUNK
BLOCK = 256
jacobian_weight = 32.0
f32 = jnp.float32
bf16 = jnp.bfloat16


def z_index(z):
    return (z % 2) * 2 + z // 2


def z_shift(block, d):
    return lax.ppermute(block, Z, [(z_index(z), z_index((z + d) % 4)) for z in range(4)])


def z_facing(block):
    return lax.ppermute(block, Z, [(t, 3 - t) for t in range(4)])


def ring_shift(block, axis, d):
    return lax.ppermute(block, axis, [(i, (i + d) % 4) for i in range(4)])


def core_swap(block):
    return lax.ppermute(block, "core", [(0, 1), (1, 0)])


def slopes(linear):
    squash = jax.nn.sigmoid(linear)
    first = squash * (1.0 + linear * (1.0 - squash))
    second = squash * (1.0 - squash) * (2.0 + linear * (1.0 - 2.0 * squash))
    return linear * squash, first, second


def per_row(top, first):
    return [top[:TANGENTS] * first[0:1], top[TANGENTS : 2 * TANGENTS] * first[1:2]]


def whole_spec(shape):
    return pl.BlockSpec(shape, lambda i, place: (0,) * len(shape))


def forward_kernel(later, final, place, rows, own, *refs):
    refs = list(refs)
    count = 4 if later else 2
    other, refs = refs[:count], refs[count:]
    if later:
        carried, refs = refs[0], refs[1:]
        if final:
            arrived, refs = refs[0], refs[1:]
            refs = refs[3:]
        else:
            refs = refs[4:]
    w_first, w_last = refs[-2:]
    outs = refs[:-2]
    tangents, picked_out, linears = outs[:3]

    @pl.when(pl.program_id(0) == 0)
    def _():
        if later:
            top = jnp.concatenate([other[0][...], other[1][...]], axis=1)
            bottom = jnp.concatenate([other[2][...], other[3][...]], axis=1)
            theirs = jnp.concatenate([top, bottom], axis=0)
        else:
            theirs = jnp.concatenate([other[0][...], other[1][...]], axis=1)
        layer = place[4]
        w_first[...] = jnp.where(layer == 0, own[...], theirs)
        w_last[...] = jnp.where(layer == 0, theirs, own[...])
        if not final:
            outs[3][...] = w_last[...]

    picked = jnp.dot(rows[...], w_first[...], preferred_element_type=f32)
    parts = []
    for c in range(2):
        part = picked[c * CHUNK : (c + 1) * CHUNK]
        linear = part[2 * TANGENTS :]
        hidden, first, _ = slopes(linear)
        parts += per_row(part, first) + [hidden]
        linears[c * 16 : (c + 1) * 16, :] = linear
    tangent = jnp.concatenate(parts, axis=0).astype(bf16)
    tangents[...] = tangent
    picked_out[...] = picked.astype(bf16)
    total = lax.dot_general(
        tangent, w_last[...], (((1,), (1,)), ((), ())), preferred_element_type=f32
    )
    if later:
        total = total + carried[...]
    if not final:
        outs[4][...] = total.astype(outs[4].dtype)
        return
    total = total + arrived[...].astype(f32)
    chunks = outs[3:]

    @pl.when(pl.program_id(0) == 0)
    def _():
        chunks[0][...] = total[:CHUNK]
        chunks[1][...] = total[CHUNK:].astype(bf16)

    @pl.when(pl.program_id(0) == 1)
    def _():
        chunks[2][...] = total[:CHUNK].astype(bf16)
        chunks[3][...] = total[CHUNK:].astype(bf16)


def forward(place, rows, weight, other, carried=None, arrived=None, saved=None, final=False):
    later = carried is not None
    at = 1 if later else 0
    step = 2 * CHUNK
    row_spec = pl.BlockSpec((step, REDUCED), lambda i, place: (i, 0))
    half_spec = pl.BlockSpec((step, HALF), lambda i, place: (i, place[2 + at]))
    in_specs = [row_spec, pl.BlockSpec((REDUCED, HALF), lambda i, place: (0, place[at]))]
    in_specs += [whole_spec(o.shape) for o in other]
    args = [rows, weight, *other]
    out_specs = [half_spec, half_spec]
    out_specs.append(pl.BlockSpec((32, HALF), lambda i, place: (i, place[2 + at])))
    out_shape = [
        jax.ShapeDtypeStruct((GROUP, COLS), bf16),
        jax.ShapeDtypeStruct((GROUP, COLS), bf16),
        jax.ShapeDtypeStruct((64, COLS), f32),
    ]
    if not final:
        out_specs.append(pl.BlockSpec((REDUCED, HALF), lambda i, place: (0, place[2 + at])))
        out_shape.append(jax.ShapeDtypeStruct((REDUCED, COLS), bf16))
        out_specs.append(row_spec)
        out_shape.append(jax.ShapeDtypeStruct((GROUP, REDUCED), bf16 if later else f32))
    else:
        out_specs += [whole_spec((CHUNK, REDUCED))] * 4
        out_shape.append(jax.ShapeDtypeStruct((CHUNK, REDUCED), f32))
        out_shape += [jax.ShapeDtypeStruct((CHUNK, REDUCED), bf16)] * 3
    aliases = {}
    if later:
        in_specs.append(row_spec)
        args.append(carried)
        if final:
            in_specs.append(row_spec)
            args.append(arrived)
        for k, s in enumerate(saved):
            aliases[1 + len(args)] = k
            in_specs.append(pl.BlockSpec(memory_space=pl.ANY))
            args.append(s)
    return pl.pallas_call(
        lambda *refs: forward_kernel(later, final, *refs),
        grid_spec=pltpu.PrefetchScalarGridSpec(
            num_scalar_prefetch=1,
            grid=(2,),
            in_specs=in_specs,
            out_specs=out_specs,
            scratch_shapes=[pltpu.VMEM((REDUCED, HALF), bf16)] * 2,
        ),
        out_shape=out_shape,
        input_output_aliases=aliases,
        compiler_params=pltpu.CompilerParams(dimension_semantics=("arbitrary",)),
        cost_estimate=pl.CostEstimate(
            flops=4 * GROUP * REDUCED * HALF, bytes_accessed=4 * REDUCED * COLS, transcendentals=0
        ),
    )(place, *args)


def transpose_into(target, whole, at_x, at_y, x_major):
    for k in range(2 * GROUP // 128):
        turned = whole[k * 128 : (k + 1) * 128, :].T
        for g in range(16):
            f = lax.rem(g // 4 - at_x + 4, 4)
            e = lax.rem(g % 4 - at_y + 4, 4)
            row = f * 128 + e * 32 if x_major else e * 128 + f * 32
            span = pl.ds(pl.multiple_of(row, 32), 32)
            target[span, k * 128 : (k + 1) * 128] = turned[g * 32 : (g + 1) * 32]


def last_kernel(place, near, far, *refs):
    misfits, outs, misfit_t = refs[:8], refs[8:12], refs[12]

    @pl.when(pl.program_id(0) == 0)
    def _():
        whole = jnp.concatenate([m[...] for m in misfits], axis=0)
        transpose_into(misfit_t, whole, place[5], place[6], True)

    tangents = jnp.concatenate([near[...], far[...]], axis=0)
    total = jnp.dot(misfit_t[...], tangents, preferred_element_type=f32).astype(bf16)
    for d in range(4):
        outs[d][...] = total[d * 128 : (d + 1) * 128]


def first_kernel(place, rows_near, rows_far, near, far, lin_near, lin_far, w_last, *refs):
    misfits, outs, rows_t, cotangents = refs[:8], refs[8:12], refs[12], refs[13]

    @pl.when(pl.program_id(0) == 0)
    def _():
        whole = jnp.concatenate([rows_near[...], rows_far[...]], axis=0)
        transpose_into(rows_t, whole, place[5], place[6], False)

    for c in range(8):
        pair = jnp.dot(misfits[c][...], w_last[...], preferred_element_type=f32)
        back = pair.astype(bf16).astype(f32)
        picked = (near, far)[c // 4][pl.ds((c % 4) * CHUNK, 2 * TANGENTS), :].astype(f32)
        linear = (lin_near, lin_far)[c // 4][pl.ds((c % 4) * 16, 16), :]
        _, first, second = slopes(linear)
        joint = back[: 2 * TANGENTS] * picked
        projected = jnp.concatenate(
            [
                jnp.sum(joint[:TANGENTS], axis=0, keepdims=True),
                jnp.sum(joint[TANGENTS:], axis=0, keepdims=True),
                jnp.zeros((14, BLOCK), f32),
            ],
            axis=0,
        )
        before = back[2 * TANGENTS :] * first + second * projected
        cotangents[pl.ds(c * CHUNK, CHUNK), :] = jnp.concatenate(
            per_row(back, first) + [before], axis=0
        ).astype(bf16)
    total = jnp.dot(rows_t[...], cotangents[...], preferred_element_type=f32).astype(bf16)
    for d in range(4):
        outs[d][...] = total[d * 128 : (d + 1) * 128]


def backward(kernel, place, args, specs, scratch, matmuls):
    return pl.pallas_call(
        kernel,
        grid_spec=pltpu.PrefetchScalarGridSpec(
            num_scalar_prefetch=1,
            grid=(COLS // BLOCK,),
            in_specs=specs,
            out_specs=[pl.BlockSpec((128, BLOCK), lambda j, place: (0, j))] * 4,
            scratch_shapes=scratch,
        ),
        out_shape=[jax.ShapeDtypeStruct((128, COLS), bf16)] * 4,
        compiler_params=pltpu.CompilerParams(dimension_semantics=("arbitrary",)),
        cost_estimate=pl.CostEstimate(
            flops=4 * matmuls * GROUP * REDUCED * COLS,
            bytes_accessed=4 * GROUP * COLS,
            transcendentals=0,
        ),
    )(place, *args)


def ring_sum(chunks, axis):
    got = [ring_shift(chunks[d], axis, d) for d in (2, 1, 3)]
    total = chunks[0].astype(f32)
    for g in got:
        total = total + g.astype(f32)
    return total


def shards(samples, targets, jacobian_targets, directions, plan, weights):
    at_x, at_y = lax.axis_index("x"), lax.axis_index("y")
    zl, core, zh = lax.axis_index("zl"), lax.axis_index("core"), lax.axis_index("zh")
    z = zh * 2 + zl
    parity = at_x % 2
    weight = weights[0]
    mine = (zl * 2 + core) * 2 + zh
    theirs = ((1 - zl) * 2 + core) * 2 + (1 - zh)
    place = jnp.stack(
        [mine * 2 + parity, mine * 2 + 1 - parity, parity, 1 - parity, zh, at_x, at_y]
    ).astype(jnp.int32)

    direct, passed = [], []
    for k in range(2):
        start = theirs * COLS + parity * HALF + k * BLOCK
        direct.append(z_facing(lax.dynamic_slice_in_dim(weight, start, BLOCK, 1)))
    for part, d in ((slice(0, 256), 1), (slice(256, 512), 3)):
        for k in range(2):
            passed.append(ring_shift(direct[k][part], "x", d))

    order = plan[0, :MICRO]
    inputs = jnp.take(samples, order, axis=0).astype(f32)
    chosen = jnp.take(directions, order, axis=0).astype(f32)
    small = lax.all_gather(jnp.concatenate([inputs, chosen], axis=1), ("zl", "core"))
    small = small.reshape(2, 2, 2, 2, REDUCED + TANGENTS).transpose(1, 2, 0, 3, 4)
    small = small.reshape(2, 4, 2, REDUCED + TANGENTS)
    small = jnp.where(core == 0, small, small[::-1])
    small = lax.dynamic_slice_in_dim(jnp.concatenate([small, small], axis=1), z, 4, 1)
    small = small.reshape(8, 2, REDUCED + TANGENTS)
    chosen = small[:, :, REDUCED:].reshape(8, 2 * TANGENTS).astype(jnp.int32)
    onehot = (chosen[:, :, None] == jnp.arange(REDUCED, dtype=jnp.int32)).astype(bf16)
    inputs = jnp.pad(small[:, :, :REDUCED].astype(bf16), ((0, 0), (0, 14), (0, 0)))
    rows = jnp.concatenate([onehot, inputs], axis=1)
    rows_near = rows[:4].reshape(GROUP, REDUCED)
    rows_far = rows[4:].reshape(GROUP, REDUCED)

    own_order = lax.dynamic_slice_in_dim(order, zh * 2, 2)
    target_rows = jnp.take(targets, own_order, axis=0).astype(f32)
    target_jac = jnp.take(jacobian_targets, own_order, axis=0).reshape(2 * TANGENTS, REDUCED)
    wanted = jnp.concatenate(
        [target_jac.astype(f32), jnp.pad(target_rows, ((0, 14), (0, 0)))], axis=0
    )

    *far_saved, far_carried = forward(place, rows_far, weight, direct)
    *near_saved, near_w, near_carried = forward(place, rows_near, weight, direct)
    tan_far, picked_far, lin_far, w_last, sent = forward(
        place, rows_far, weight, passed, far_carried, saved=far_saved
    )
    from_core = core_swap(sent)
    tan_near, picked_near, lin_near, *chunks = forward(
        place, rows_near, weight, passed, near_carried, from_core, near_saved, True
    )
    got = [z_shift(chunks[d], d) for d in (2, 1, 3)]
    total = chunks[0]
    for g in got:
        total = total + g.astype(f32)
    scale = jnp.where(jnp.arange(CHUNK)[:, None] < 2 * TANGENTS, jacobian_weight, 1.0)
    misfit = (scale * (total - wanted)).astype(bf16)
    near = [misfit, None, None, None]
    for d in (2, 1, 3):
        near[d] = z_shift(misfit, 4 - d)
    misfits = near + [core_swap(m) for m in near]

    whole_misfits = [whole_spec((CHUNK, REDUCED))] * 8
    columns = lambda rows: pl.BlockSpec((rows, BLOCK), lambda j, place: (0, j))
    turned = pltpu.VMEM((REDUCED, 2 * GROUP), bf16)
    grad_last = backward(
        last_kernel,
        place,
        [tan_near, tan_far, *misfits],
        [columns(GROUP), columns(GROUP), *whole_misfits],
        [turned],
        1,
    )
    grad_first = backward(
        first_kernel,
        place,
        [rows_near, rows_far, picked_near, picked_far, lin_near, lin_far, w_last, *misfits],
        [whole_spec((GROUP, REDUCED))] * 2
        + [columns(GROUP), columns(GROUP), columns(64), columns(64), columns(REDUCED)]
        + whole_misfits,
        [turned, pltpu.VMEM((2 * GROUP, BLOCK), bf16)],
        2,
    )

    last = ring_sum(grad_last, "x").astype(bf16).reshape(4, 32, COLS)
    first = ring_sum(grad_first, "y").astype(bf16).reshape(4, 32, COLS)
    last = ring_sum(last, "y")
    first = ring_sum(first, "x")

    both = jnp.stack([first.reshape(2, 2, 8, COLS), last.reshape(2, 2, 8, COLS)], axis=2)
    result = lax.all_to_all(
        both.reshape(8, 8, COLS), ("zl", "core", "zh"), split_axis=0, concat_axis=0, tiled=True
    )
    return result.transpose(1, 0, 2).reshape(1, 8, 8 * COLS)


def solution(mesh):
    torus = Mesh(mesh.devices.reshape(4, 4, 2, 2, 2), AXES)
    return jax.shard_map(
        shards,
        mesh=torus,
        in_specs=(
            P(DP, None),
            P(DP, None),
            P(DP, None, None),
            P(DP, None),
            P(DP, None),
            P("zh", None, None),
        ),
        out_specs=P("zh", DP, None),
        check_vma=False,
    )
```

```python
import jax
import jax.numpy as jnp
from jax import lax
from jax.experimental import pallas as pl
from jax.experimental.pallas import tpu as pltpu
from jax.sharding import Mesh
from jax.sharding import PartitionSpec as P

AXES = ("x", "y", "zl", "core", "zh")
DP = ("x", "y", "zl", "core")
Z = ("zl", "zh")
MICRO = 4
REDUCED = 512
COLS = 1024
BLOCK = 256
TANGENTS = 128
CHUNK = 2 * TANGENTS + 16
GROUP = 4 * CHUNK
STEP = 2 * CHUNK
jacobian_weight = 32.0
f32 = jnp.float32
bf16 = jnp.bfloat16


def z_index(z):
    return (z % 2) * 2 + z // 2


def z_shift(block, d):
    return lax.ppermute(block, Z, [(z_index(z), z_index((z + d) % 4)) for z in range(4)])


def z_facing(block):
    return lax.ppermute(block, Z, [(t, 3 - t) for t in range(4)])


def ring_shift(block, axis, d):
    return lax.ppermute(block, axis, [(i, (i + d) % 4) for i in range(4)])


def core_swap(block):
    return lax.ppermute(block, "core", [(0, 1), (1, 0)])


def slopes(linear):
    squash = jax.nn.sigmoid(linear)
    first = squash * (1.0 + linear * (1.0 - squash))
    second = squash * (1.0 - squash) * (2.0 + linear * (1.0 - 2.0 * squash))
    return linear * squash, first, second


def per_row(top, first):
    return [top[:TANGENTS] * first[0:1], top[TANGENTS : 2 * TANGENTS] * first[1:2]]


def whole_spec(shape):
    return pl.BlockSpec(shape, lambda i, place: (0,) * len(shape))


def own_specs():
    return [pl.BlockSpec((REDUCED, BLOCK), lambda i, place, k=k: (0, place[k])) for k in range(4)]


def forward_kernel(final, place, rows, *refs):
    own, other, refs = refs[:4], refs[4:8], refs[8:]
    if final:
        arrived, refs = refs[0], refs[1:]
    w_first, w_last = refs[-2:]
    outs = refs[:-2]

    @pl.when(pl.program_id(0) == 0)
    def _():
        here = place[4] == 0
        for k in range(4):
            span = slice(k * BLOCK, (k + 1) * BLOCK)
            w_first[:, span] = jnp.where(here, own[k][...], other[k][...])
            w_last[:, span] = jnp.where(here, other[k][...], own[k][...])

    picked = jnp.dot(rows[...], w_first[...], preferred_element_type=f32)
    parts = []
    for c in range(2):
        part = picked[c * CHUNK : (c + 1) * CHUNK]
        hidden, first, _ = slopes(part[2 * TANGENTS :])
        parts += per_row(part, first) + [hidden]
    tangent = jnp.concatenate(parts, axis=0).astype(bf16)
    total = lax.dot_general(
        tangent, w_last[...], (((1,), (1,)), ((), ())), preferred_element_type=f32
    )
    if not final:
        outs[0][...] = total.astype(bf16)
        return
    total = total + arrived[...].astype(f32)

    @pl.when(pl.program_id(0) == 0)
    def _():
        outs[0][...] = total[:CHUNK]
        outs[1][...] = total[CHUNK:].astype(bf16)

    @pl.when(pl.program_id(0) == 1)
    def _():
        outs[2][...] = total[:CHUNK].astype(bf16)
        outs[3][...] = total[CHUNK:].astype(bf16)


def forward(place, rows, weight, other, arrived=None):
    final = arrived is not None
    base = 0 if final else 2
    in_specs = [pl.BlockSpec((STEP, REDUCED), lambda i, place: (i + base, 0)), *own_specs()]
    in_specs += [whole_spec((REDUCED, BLOCK))] * 4
    args = [rows, weight, weight, weight, weight, *other]
    out_specs = pl.BlockSpec((STEP, REDUCED), lambda i, place: (i, 0))
    out_shape = jax.ShapeDtypeStruct((GROUP, REDUCED), bf16)
    if final:
        in_specs.append(out_specs)
        args.append(arrived)
        out_specs = [whole_spec((CHUNK, REDUCED))] * 4
        out_shape = [jax.ShapeDtypeStruct((CHUNK, REDUCED), f32)]
        out_shape += [jax.ShapeDtypeStruct((CHUNK, REDUCED), bf16)] * 3
    return pl.pallas_call(
        lambda *refs: forward_kernel(final, *refs),
        grid_spec=pltpu.PrefetchScalarGridSpec(
            num_scalar_prefetch=1,
            grid=(2,),
            in_specs=in_specs,
            out_specs=out_specs,
            scratch_shapes=[pltpu.VMEM((REDUCED, COLS), bf16)] * 2,
        ),
        out_shape=out_shape,
        compiler_params=pltpu.CompilerParams(dimension_semantics=("arbitrary",)),
        cost_estimate=pl.CostEstimate(
            flops=4 * GROUP * REDUCED * COLS, bytes_accessed=4 * REDUCED * COLS, transcendentals=0
        ),
    )(place, *args)


def backward_kernel(place, rows, own, *refs):
    other, misfits, out = refs[:4], refs[4:12], refs[12]
    tangents, cotangents = refs[13:]
    step = pl.program_id(0)
    theirs = other[3][...]
    for k in range(3):
        theirs = jnp.where(step == k, other[k][...], theirs)
    here = place[4] == 0
    w_first = jnp.where(here, own[...], theirs)
    w_last = jnp.where(here, theirs, own[...])
    for c in range(8):
        span = pl.ds(c * CHUNK, CHUNK)
        picked = jnp.dot(rows[span, :], w_first, preferred_element_type=f32)
        hidden, first, second = slopes(picked[2 * TANGENTS :])
        tangents[span, :] = jnp.concatenate(per_row(picked, first) + [hidden], axis=0).astype(bf16)
        back = jnp.dot(misfits[c][...], w_last, preferred_element_type=f32)
        back = back.astype(bf16).astype(f32)
        joint = back[: 2 * TANGENTS] * picked[: 2 * TANGENTS]
        projected = jnp.concatenate(
            [
                jnp.sum(joint[:TANGENTS], axis=0, keepdims=True),
                jnp.sum(joint[TANGENTS:], axis=0, keepdims=True),
                jnp.zeros((14, BLOCK), f32),
            ],
            axis=0,
        )
        before = back[2 * TANGENTS :] * first + second * projected
        cotangents[span, :] = jnp.concatenate(per_row(back, first) + [before], axis=0).astype(bf16)
    over_rows = (((0,), (0,)), ((), ()))
    whole = jnp.concatenate([m[...] for m in misfits], axis=0)
    last = lax.dot_general(whole, tangents[...], over_rows, preferred_element_type=f32)
    first = lax.dot_general(rows[...], cotangents[...], over_rows, preferred_element_type=f32)
    out[:, 0] = first.astype(bf16).reshape(64, 8, BLOCK)
    out[:, 1] = last.astype(bf16).reshape(64, 8, BLOCK)


def backward(place, rows, misfits, weight, other):
    return pl.pallas_call(
        backward_kernel,
        grid_spec=pltpu.PrefetchScalarGridSpec(
            num_scalar_prefetch=1,
            grid=(4,),
            in_specs=[
                whole_spec((2 * GROUP, REDUCED)),
                pl.BlockSpec((REDUCED, BLOCK), lambda j, place: (0, place[j])),
                *[whole_spec((REDUCED, BLOCK))] * 4,
                *[whole_spec((CHUNK, REDUCED))] * 8,
            ],
            out_specs=pl.BlockSpec((64, 2, 8, BLOCK), lambda j, place: (0, 0, 0, place[5 + j])),
            scratch_shapes=[pltpu.VMEM((2 * GROUP, BLOCK), bf16)] * 2,
        ),
        out_shape=jax.ShapeDtypeStruct((64, 2, 8, COLS), bf16),
        compiler_params=pltpu.CompilerParams(dimension_semantics=("arbitrary",)),
        cost_estimate=pl.CostEstimate(
            flops=16 * GROUP * REDUCED * COLS, bytes_accessed=4 * REDUCED * COLS, transcendentals=0
        ),
    )(place, rows, weight, *other, *misfits)


def total_kernel(pieces, out):
    for u in range(2):
        total = pieces[0, u].astype(f32)
        for k in range(1, 16):
            total = total + pieces[k, u].astype(f32)
        out[0, :, u * COLS : (u + 1) * COLS] = total


def total_of(pieces):
    return pl.pallas_call(
        total_kernel,
        grid=(4,),
        in_specs=[pl.BlockSpec((16, 2, 8, COLS), lambda i: (0, i, 0, 0))],
        out_specs=pl.BlockSpec((1, 8, 2 * COLS), lambda i: (0, 0, i)),
        out_shape=jax.ShapeDtypeStruct((1, 8, 8 * COLS), f32),
        compiler_params=pltpu.CompilerParams(dimension_semantics=("arbitrary",)),
    )(pieces)


def shards(samples, targets, jacobian_targets, directions, plan, weights):
    at_x, at_y = lax.axis_index("x"), lax.axis_index("y")
    zl, core, zh = lax.axis_index("zl"), lax.axis_index("core"), lax.axis_index("zh")
    z = zh * 2 + zl
    kind = (at_x + 2 * at_y) % 4
    weight = weights[0]
    mine = (zl * 2 + core) * 2 + zh
    theirs = ((1 - zl) * 2 + core) * 2 + (1 - zh)
    turn = [(kind + k) % 4 for k in range(4)]
    place = jnp.stack([mine * 4 + t for t in turn] + [zh] + turn).astype(jnp.int32)

    quarter = lax.dynamic_slice_in_dim(weight, theirs * COLS + kind * BLOCK, BLOCK, 1)
    direct = z_facing(quarter)

    order = plan[0, :MICRO]
    inputs = jnp.take(samples, order, axis=0).astype(f32)
    chosen = jnp.take(directions, order, axis=0).astype(f32)
    packed = jnp.concatenate([inputs, chosen], axis=1)
    direct, packed = lax.optimization_barrier((direct, packed))
    other = [
        direct,
        ring_shift(direct, "x", 3),
        ring_shift(direct, "y", 3),
        ring_shift(direct, "x", 1),
    ]
    small = lax.all_gather(packed, ("zl", "core"))
    small = small.reshape(2, 2, 2, 2, REDUCED + TANGENTS).transpose(1, 2, 0, 3, 4)
    small = small.reshape(2, 4, 2, REDUCED + TANGENTS)
    small = jnp.where(core == 0, small, small[::-1])
    small = lax.dynamic_slice_in_dim(jnp.concatenate([small, small], axis=1), z, 4, 1)
    small = small.reshape(8, 2, REDUCED + TANGENTS)
    chosen = small[:, :, REDUCED:].reshape(8, 2 * TANGENTS).astype(jnp.int32)
    onehot = (chosen[:, :, None] == jnp.arange(REDUCED, dtype=jnp.int32)).astype(bf16)
    inputs = jnp.pad(small[:, :, :REDUCED].astype(bf16), ((0, 0), (0, 14), (0, 0)))
    rows = jnp.concatenate([onehot, inputs], axis=1).reshape(2 * GROUP, REDUCED)

    own_order = lax.dynamic_slice_in_dim(order, zh * 2, 2)
    target_rows = jnp.take(targets, own_order, axis=0).astype(f32)
    target_jac = jnp.take(jacobian_targets, own_order, axis=0).reshape(2 * TANGENTS, REDUCED)
    wanted = jnp.concatenate(
        [target_jac.astype(f32), jnp.pad(target_rows, ((0, 14), (0, 0)))], axis=0
    )

    from_core = core_swap(forward(place, rows, weight, other))
    chunks = forward(place, rows, weight, other, from_core)
    got = [z_shift(chunks[d], d) for d in (2, 1, 3)]
    total = chunks[0]
    for g in got:
        total = total + g.astype(f32)
    scale = jnp.where(jnp.arange(CHUNK)[:, None] < 2 * TANGENTS, jacobian_weight, 1.0)
    misfit = (scale * (total - wanted)).astype(bf16)
    near = [misfit, None, None, None]
    for d in (2, 1, 3):
        near[d] = z_shift(misfit, 4 - d)
    misfits = near + [core_swap(m) for m in near]
    sent = backward(place, rows, misfits, weight, other)
    pieces = lax.all_to_all(
        sent.reshape(128, 8, COLS), AXES, split_axis=0, concat_axis=0, tiled=True
    )
    return total_of(pieces.reshape(16, 8, 8, COLS))


def solution(mesh):
    torus = Mesh(mesh.devices.reshape(4, 4, 2, 2, 2), AXES)
    return jax.shard_map(
        shards,
        mesh=torus,
        in_specs=(
            P(DP, None),
            P(DP, None),
            P(DP, None, None),
            P(DP, None),
            P(DP, None),
            P("zh", None, None),
        ),
        out_specs=P("zh", DP, None),
        check_vma=False,
    )
```

```python
import jax
import jax.numpy as jnp
from jax import lax
from jax.experimental import pallas as pl
from jax.experimental.pallas import tpu as pltpu
from jax.sharding import Mesh
from jax.sharding import PartitionSpec as P

AXES = ("x", "y", "zl", "core", "zh")
DP = ("x", "y", "zl", "core")
Z = ("zl", "zh")
MICRO = 4
REDUCED = 512
COLS = 1024
BLOCK = 256
TANGENTS = 128
CHUNK = 2 * TANGENTS + 16
GROUP = 4 * CHUNK
STEP = 2 * CHUNK
PARTS = (TANGENTS, TANGENTS + 16)
jacobian_weight = 32.0
f32 = jnp.float32
bf16 = jnp.bfloat16


def z_index(z):
    return (z % 2) * 2 + z // 2


def z_shift(block, d):
    return lax.ppermute(block, Z, [(z_index(z), z_index((z + d) % 4)) for z in range(4)])


def z_facing(block):
    return lax.ppermute(block, Z, [(t, 3 - t) for t in range(4)])


def ring_shift(block, axis, d):
    return lax.ppermute(block, axis, [(i, (i + d) % 4) for i in range(4)])


def core_swap(block):
    return lax.ppermute(block, "core", [(0, 1), (1, 0)])


def slopes(linear):
    squash = jax.nn.sigmoid(linear)
    first = squash * (1.0 + linear * (1.0 - squash))
    second = squash * (1.0 - squash) * (2.0 + linear * (1.0 - 2.0 * squash))
    return linear * squash, first, second


def per_row(top, first):
    return [top[:TANGENTS] * first[0:1], top[TANGENTS : 2 * TANGENTS] * first[1:2]]


def whole_spec(shape):
    return pl.BlockSpec(shape, lambda i, place: (0,) * len(shape))


def own_specs():
    return [pl.BlockSpec((REDUCED, BLOCK), lambda i, place, k=k: (0, place[k])) for k in range(4)]


def forward_kernel(final, place, rows, *refs):
    own, other, refs = refs[:4], refs[4:8], refs[8:]
    if final:
        arrived, refs = refs[0], refs[1:]
    w_first, w_last = refs[-2:]
    outs = refs[:-2]

    @pl.when(pl.program_id(0) == 0)
    def _():
        here = place[4] == 0
        for k in range(4):
            span = slice(k * BLOCK, (k + 1) * BLOCK)
            w_first[:, span] = jnp.where(here, own[k][...], other[k][...])
            w_last[:, span] = jnp.where(here, other[k][...], own[k][...])

    picked = jnp.dot(rows[...], w_first[...], preferred_element_type=f32)
    parts = []
    for c in range(2):
        part = picked[c * CHUNK : (c + 1) * CHUNK]
        hidden, first, _ = slopes(part[2 * TANGENTS :])
        parts += per_row(part, first) + [hidden]
    tangent = jnp.concatenate(parts, axis=0).astype(bf16)
    total = lax.dot_general(
        tangent, w_last[...], (((1,), (1,)), ((), ())), preferred_element_type=f32
    )
    if not final:
        outs[0][...] = total.astype(bf16)
        return
    total = total + arrived[...].astype(f32)
    for step in range(2):

        @pl.when(pl.program_id(0) == step)
        def _():
            for c in range(2):
                at = c * CHUNK
                for part in PARTS:
                    out = outs[2 * (2 * step + c) + (part > TANGENTS)]
                    out[...] = total[at : at + part].astype(out.dtype)
                    at += part


def forward(place, rows, weight, other, arrived=None):
    final = arrived is not None
    base = 0 if final else 2
    in_specs = [pl.BlockSpec((STEP, REDUCED), lambda i, place: (i + base, 0)), *own_specs()]
    in_specs += [whole_spec((REDUCED, BLOCK))] * 4
    args = [rows, weight, weight, weight, weight, *other]
    out_specs = pl.BlockSpec((STEP, REDUCED), lambda i, place: (i, 0))
    out_shape = jax.ShapeDtypeStruct((GROUP, REDUCED), bf16)
    if final:
        in_specs.append(out_specs)
        args.append(arrived)
        out_specs = [whole_spec((part, REDUCED)) for part in PARTS] * 4
        out_shape = [jax.ShapeDtypeStruct((part, REDUCED), f32) for part in PARTS]
        out_shape += [jax.ShapeDtypeStruct((part, REDUCED), bf16) for part in PARTS] * 3
    return pl.pallas_call(
        lambda *refs: forward_kernel(final, *refs),
        grid_spec=pltpu.PrefetchScalarGridSpec(
            num_scalar_prefetch=1,
            grid=(2,),
            in_specs=in_specs,
            out_specs=out_specs,
            scratch_shapes=[pltpu.VMEM((REDUCED, COLS), bf16)] * 2,
        ),
        out_shape=out_shape,
        compiler_params=pltpu.CompilerParams(dimension_semantics=("arbitrary",)),
        cost_estimate=pl.CostEstimate(
            flops=4 * GROUP * REDUCED * COLS, bytes_accessed=4 * REDUCED * COLS, transcendentals=0
        ),
    )(place, *args)


def backward_kernel(place, rows, own, *refs):
    other, misfits, out = refs[:4], refs[4:20], refs[20]
    tangents, cotangents = refs[21:]
    whole = jnp.concatenate([m[...] for m in misfits], axis=0)
    step = pl.program_id(0)
    theirs = other[3][...]
    for k in range(3):
        theirs = jnp.where(step == k, other[k][...], theirs)
    here = place[4] == 0
    w_first = jnp.where(here, own[...], theirs)
    w_last = jnp.where(here, theirs, own[...])
    for c in range(8):
        span = pl.ds(c * CHUNK, CHUNK)
        picked = jnp.dot(rows[span, :], w_first, preferred_element_type=f32)
        hidden, first, second = slopes(picked[2 * TANGENTS :])
        tangents[span, :] = jnp.concatenate(per_row(picked, first) + [hidden], axis=0).astype(bf16)
        misfit = jnp.concatenate([misfits[2 * c][...], misfits[2 * c + 1][...]], axis=0)
        back = jnp.dot(misfit, w_last, preferred_element_type=f32)
        back = back.astype(bf16).astype(f32)
        joint = back[: 2 * TANGENTS] * picked[: 2 * TANGENTS]
        projected = jnp.concatenate(
            [
                jnp.sum(joint[:TANGENTS], axis=0, keepdims=True),
                jnp.sum(joint[TANGENTS:], axis=0, keepdims=True),
                jnp.zeros((14, BLOCK), f32),
            ],
            axis=0,
        )
        before = back[2 * TANGENTS :] * first + second * projected
        cotangents[span, :] = jnp.concatenate(per_row(back, first) + [before], axis=0).astype(bf16)
    over_rows = (((0,), (0,)), ((), ()))
    last = lax.dot_general(whole, tangents[...], over_rows, preferred_element_type=f32)
    first = lax.dot_general(rows[...], cotangents[...], over_rows, preferred_element_type=f32)
    out[:, 0] = first.astype(bf16).reshape(64, 8, BLOCK)
    out[:, 1] = last.astype(bf16).reshape(64, 8, BLOCK)


def backward(place, rows, misfits, weight, other):
    return pl.pallas_call(
        backward_kernel,
        grid_spec=pltpu.PrefetchScalarGridSpec(
            num_scalar_prefetch=1,
            grid=(4,),
            in_specs=[
                whole_spec((2 * GROUP, REDUCED)),
                pl.BlockSpec((REDUCED, BLOCK), lambda j, place: (0, place[j])),
                *[whole_spec((REDUCED, BLOCK))] * 4,
                *[whole_spec((part, REDUCED)) for part in PARTS] * 8,
            ],
            out_specs=pl.BlockSpec((64, 2, 8, BLOCK), lambda j, place: (0, 0, 0, place[5 + j])),
            scratch_shapes=[pltpu.VMEM((2 * GROUP, BLOCK), bf16)] * 2,
        ),
        out_shape=jax.ShapeDtypeStruct((64, 2, 8, COLS), bf16),
        compiler_params=pltpu.CompilerParams(dimension_semantics=("arbitrary",)),
        cost_estimate=pl.CostEstimate(
            flops=16 * GROUP * REDUCED * COLS, bytes_accessed=4 * REDUCED * COLS, transcendentals=0
        ),
    )(place, rows, weight, *other, *misfits)


def total_kernel(pieces, out):
    for u in range(2):
        total = pieces[0, u].astype(f32)
        for k in range(1, 16):
            total = total + pieces[k, u].astype(f32)
        out[0, :, u * COLS : (u + 1) * COLS] = total


def total_of(pieces):
    return pl.pallas_call(
        total_kernel,
        grid=(4,),
        in_specs=[pl.BlockSpec((16, 2, 8, COLS), lambda i: (0, i, 0, 0))],
        out_specs=pl.BlockSpec((1, 8, 2 * COLS), lambda i: (0, 0, i)),
        out_shape=jax.ShapeDtypeStruct((1, 8, 8 * COLS), f32),
        compiler_params=pltpu.CompilerParams(dimension_semantics=("arbitrary",)),
    )(pieces)


def shards(samples, targets, jacobian_targets, directions, plan, weights):
    at_x, at_y = lax.axis_index("x"), lax.axis_index("y")
    zl, core, zh = lax.axis_index("zl"), lax.axis_index("core"), lax.axis_index("zh")
    z = zh * 2 + zl
    kind = (at_x + 2 * at_y) % 4
    weight = weights[0]
    mine = (zl * 2 + core) * 2 + zh
    theirs = ((1 - zl) * 2 + core) * 2 + (1 - zh)
    turn = [(kind + k) % 4 for k in range(4)]
    place = jnp.stack([mine * 4 + t for t in turn] + [zh] + turn).astype(jnp.int32)

    quarter = lax.dynamic_slice_in_dim(weight, theirs * COLS + kind * BLOCK, BLOCK, 1)
    direct = z_facing(quarter)

    order = plan[0, :MICRO]
    inputs = jnp.take(samples, order, axis=0).astype(f32)
    chosen = jnp.take(directions, order, axis=0).astype(f32)
    packed = jnp.concatenate([inputs, chosen], axis=1)
    swapped = core_swap(packed)
    direct, packed, swapped = lax.optimization_barrier((direct, packed, swapped))
    other = [
        direct,
        ring_shift(direct, "x", 3),
        ring_shift(direct, "y", 3),
        ring_shift(direct, "x", 1),
    ]
    pair = jnp.concatenate([packed, swapped], axis=0)
    beside = lax.ppermute(pair, "zl", [(0, 1), (1, 0)])
    low = jnp.where(zl == 0, pair, beside).reshape(2, 2, 2, REDUCED + TANGENTS)
    high = jnp.where(zl == 0, beside, pair).reshape(2, 2, 2, REDUCED + TANGENTS)
    small = jnp.stack([low, high], axis=2).reshape(2, 4, 2, REDUCED + TANGENTS)
    small = lax.dynamic_slice_in_dim(jnp.concatenate([small, small], axis=1), z, 4, 1)
    small = small.reshape(8, 2, REDUCED + TANGENTS)
    chosen = small[:, :, REDUCED:].reshape(8, 2 * TANGENTS).astype(jnp.int32)
    onehot = (chosen[:, :, None] == jnp.arange(REDUCED, dtype=jnp.int32)).astype(bf16)
    inputs = jnp.pad(small[:, :, :REDUCED].astype(bf16), ((0, 0), (0, 14), (0, 0)))
    rows = jnp.concatenate([onehot, inputs], axis=1).reshape(2 * GROUP, REDUCED)

    own_order = lax.dynamic_slice_in_dim(order, zh * 2, 2)
    target_rows = jnp.take(targets, own_order, axis=0).astype(f32)
    target_jac = jnp.take(jacobian_targets, own_order, axis=0).reshape(2 * TANGENTS, REDUCED)
    wanted = [
        target_jac[:TANGENTS].astype(f32),
        jnp.concatenate(
            [target_jac[TANGENTS:].astype(f32), jnp.pad(target_rows, ((0, 14), (0, 0)))], axis=0
        ),
    ]

    from_core = core_swap(forward(place, rows, weight, other))
    from_core, wanted = lax.optimization_barrier((from_core, wanted))
    parts = forward(place, rows, weight, other, from_core)
    got = [[z_shift(parts[2 * d + p], d) for d in (2, 1, 3)] for p in range(2)]
    near = [[], []]
    for p in range(2):
        total = parts[p]
        for g in got[p]:
            total = total + g.astype(f32)
        scale = jnp.where(jnp.arange(PARTS[p])[:, None] < TANGENTS, jacobian_weight, 1.0)
        misfit = (scale * (total - wanted[p])).astype(bf16)
        near[p] = [misfit, None, None, None]
        for d in (2, 1, 3):
            near[p][d] = z_shift(misfit, 4 - d)
    near = [near[p][d] for d in range(4) for p in range(2)]
    misfits = near + [core_swap(m) for m in near]
    sent = backward(place, rows, misfits, weight, other)
    pieces = lax.all_to_all(
        sent.reshape(128, 8, COLS), AXES, split_axis=0, concat_axis=0, tiled=True
    )
    return total_of(pieces.reshape(16, 8, 8, COLS))


def solution(mesh):
    torus = Mesh(mesh.devices.reshape(4, 4, 2, 2, 2), AXES)
    return jax.shard_map(
        shards,
        mesh=torus,
        in_specs=(
            P(DP, None),
            P(DP, None),
            P(DP, None, None),
            P(DP, None),
            P(DP, None),
            P("zh", None, None),
        ),
        out_specs=P("zh", DP, None),
        check_vma=False,
    )
```

```python
import jax
import jax.numpy as jnp
from jax import lax
from jax.experimental import pallas as pl
from jax.experimental.pallas import tpu as pltpu
from jax.sharding import Mesh
from jax.sharding import PartitionSpec as P

AXES = ("x", "y", "zl", "core", "zh")
DP = ("x", "y", "zl", "core")
Z = ("zl", "zh")
MICRO = 4
REDUCED = 512
COLS = 1024
BLOCK = 256
TANGENTS = 128
CHUNK = 2 * TANGENTS + 16
GROUP = 4 * CHUNK
STEP = 2 * CHUNK
LIMIT = 24 * 2**20
jacobian_weight = 32.0
f32 = jnp.float32
bf16 = jnp.bfloat16


def z_index(z):
    return (z % 2) * 2 + z // 2


def z_shift(block, d):
    return lax.ppermute(block, Z, [(z_index(z), z_index((z + d) % 4)) for z in range(4)])


def z_facing(block):
    return lax.ppermute(block, Z, [(t, 3 - t) for t in range(4)])


def ring_shift(block, axis, d):
    return lax.ppermute(block, axis, [(i, (i + d) % 4) for i in range(4)])


def core_swap(block):
    return lax.ppermute(block, "core", [(0, 1), (1, 0)])


def slopes(linear):
    squash = jax.nn.sigmoid(linear)
    first = squash * (1.0 + linear * (1.0 - squash))
    second = squash * (1.0 - squash) * (2.0 + linear * (1.0 - 2.0 * squash))
    return linear * squash, first, second


def per_row(top, first):
    return [top[:TANGENTS] * first[0:1], top[TANGENTS : 2 * TANGENTS] * first[1:2]]


def whole_spec(shape):
    return pl.BlockSpec(shape, lambda i, place: (0,) * len(shape))


def own_specs():
    return [pl.BlockSpec((REDUCED, BLOCK), lambda i, place, k=k: (0, place[k])) for k in range(4)]


def forward_kernel(final, place, rows, *refs):
    own, other, refs = refs[:4], refs[4:8], refs[8:]
    if final:
        arrived, refs = refs[0], refs[1:]
    w_first, w_last = refs[-2:]
    outs = refs[:-2]

    @pl.when(pl.program_id(0) == 0)
    def _():
        here = place[4] == 0
        for k in range(4):
            span = slice(k * BLOCK, (k + 1) * BLOCK)
            w_first[:, span] = jnp.where(here, own[k][...], other[k][...])
            w_last[:, span] = jnp.where(here, other[k][...], own[k][...])

    picked = jnp.dot(rows[...], w_first[...], preferred_element_type=f32)
    parts = []
    for c in range(2):
        part = picked[c * CHUNK : (c + 1) * CHUNK]
        hidden, first, _ = slopes(part[2 * TANGENTS :])
        parts += per_row(part, first) + [hidden]
    tangent = jnp.concatenate(parts, axis=0).astype(bf16)
    total = lax.dot_general(
        tangent, w_last[...], (((1,), (1,)), ((), ())), preferred_element_type=f32
    )
    if not final:
        outs[0][...] = total.astype(bf16)
        return
    total = total + arrived[...].astype(f32)
    for step in range(2):

        @pl.when(pl.program_id(0) == step)
        def _():
            for c in range(2):
                out = outs[2 * step + c]
                out[...] = total[c * CHUNK : (c + 1) * CHUNK].astype(out.dtype)


def forward(place, rows, own, other, arrived=None):
    final = arrived is not None
    base = 0 if final else 2
    in_specs = [pl.BlockSpec((STEP, REDUCED), lambda i, place: (i + base, 0)), *own_specs()]
    in_specs += [whole_spec((REDUCED, BLOCK))] * 4
    args = [rows, own, own, own, own, *other]
    out_specs = pl.BlockSpec((STEP, REDUCED), lambda i, place: (i, 0))
    out_shape = jax.ShapeDtypeStruct((GROUP, REDUCED), bf16)
    if final:
        in_specs.append(out_specs)
        args.append(arrived)
        out_specs = [whole_spec((CHUNK, REDUCED))] * 4
        out_shape = [jax.ShapeDtypeStruct((CHUNK, REDUCED), f32)]
        out_shape += [jax.ShapeDtypeStruct((CHUNK, REDUCED), bf16)] * 3
    return pl.pallas_call(
        lambda *refs: forward_kernel(final, *refs),
        grid_spec=pltpu.PrefetchScalarGridSpec(
            num_scalar_prefetch=1,
            grid=(2,),
            in_specs=in_specs,
            out_specs=out_specs,
            scratch_shapes=[pltpu.VMEM((REDUCED, COLS), bf16)] * 2,
        ),
        out_shape=out_shape,
        compiler_params=pltpu.CompilerParams(
            dimension_semantics=("arbitrary",), vmem_limit_bytes=LIMIT
        ),
        cost_estimate=pl.CostEstimate(
            flops=4 * GROUP * REDUCED * COLS, bytes_accessed=4 * REDUCED * COLS, transcendentals=0
        ),
    )(place, *args)


def piece_of(step, pieces):
    chosen = pieces[3][...]
    for k in range(3):
        chosen = jnp.where(step == k, pieces[k][...], chosen)
    return chosen


def prepare_kernel(place, rows, own, *refs):
    other, (picked_out, tangents, linears) = refs[:4], refs[4:]
    theirs = piece_of(pl.program_id(0), other)
    w_first = jnp.where(place[4] == 0, own[...], theirs)
    for c in range(0, 8, 2):
        span = pl.ds(c * CHUNK, STEP)
        picked = jnp.dot(rows[span, :], w_first, preferred_element_type=f32)
        picked_out[span, :] = picked.astype(bf16)
        parts = []
        for e in range(2):
            part = picked[e * CHUNK : (e + 1) * CHUNK]
            linear = part[2 * TANGENTS :]
            hidden, first, _ = slopes(linear)
            parts += per_row(part, first) + [hidden]
            linears[pl.ds((c + e) * 16, 16), :] = linear
        tangents[span, :] = jnp.concatenate(parts, axis=0).astype(bf16)


def prepare(place, rows, own, other):
    columns = lambda height: pl.BlockSpec((height, BLOCK), lambda j, place: (0, j))
    return pl.pallas_call(
        prepare_kernel,
        grid_spec=pltpu.PrefetchScalarGridSpec(
            num_scalar_prefetch=1,
            grid=(4,),
            in_specs=[
                whole_spec((2 * GROUP, REDUCED)),
                pl.BlockSpec((REDUCED, BLOCK), lambda j, place: (0, place[j])),
                *[whole_spec((REDUCED, BLOCK))] * 4,
            ],
            out_specs=[columns(2 * GROUP), columns(2 * GROUP), columns(128)],
        ),
        out_shape=[
            jax.ShapeDtypeStruct((2 * GROUP, COLS), bf16),
            jax.ShapeDtypeStruct((2 * GROUP, COLS), bf16),
            jax.ShapeDtypeStruct((128, COLS), f32),
        ],
        compiler_params=pltpu.CompilerParams(
            dimension_semantics=("arbitrary",), vmem_limit_bytes=LIMIT
        ),
        cost_estimate=pl.CostEstimate(
            flops=4 * GROUP * REDUCED * COLS, bytes_accessed=4 * REDUCED * COLS, transcendentals=0
        ),
    )(place, rows, own, *other)


def backward_kernel(place, rows, picked, tangents, linears, own, *refs):
    other, misfits, out, cotangents = refs[:4], refs[4:12], refs[12], refs[13]
    theirs = piece_of(pl.program_id(0), other)
    w_last = jnp.where(place[4] == 0, theirs, own[...])
    for c in range(8):
        span = pl.ds(c * CHUNK, CHUNK)
        back = jnp.dot(misfits[c][...], w_last, preferred_element_type=f32)
        back = back.astype(bf16).astype(f32)
        _, first, second = slopes(linears[pl.ds(c * 16, 16), :])
        joint = back[: 2 * TANGENTS] * picked[pl.ds(c * CHUNK, 2 * TANGENTS), :].astype(f32)
        projected = jnp.concatenate(
            [
                jnp.sum(joint[:TANGENTS], axis=0, keepdims=True),
                jnp.sum(joint[TANGENTS:], axis=0, keepdims=True),
                jnp.zeros((14, BLOCK), f32),
            ],
            axis=0,
        )
        before = back[2 * TANGENTS :] * first + second * projected
        cotangents[span, :] = jnp.concatenate(per_row(back, first) + [before], axis=0).astype(bf16)
    over_rows = (((0,), (0,)), ((), ()))
    whole = jnp.concatenate([m[...] for m in misfits], axis=0)
    last = lax.dot_general(whole, tangents[...], over_rows, preferred_element_type=f32)
    first = lax.dot_general(rows[...], cotangents[...], over_rows, preferred_element_type=f32)
    out[:, 0] = first.astype(bf16).reshape(64, 8, BLOCK)
    out[:, 1] = last.astype(bf16).reshape(64, 8, BLOCK)


def backward(place, rows, prepared, own, other, misfits):
    columns = lambda height: pl.BlockSpec((height, BLOCK), lambda j, place: (0, j))
    return pl.pallas_call(
        backward_kernel,
        grid_spec=pltpu.PrefetchScalarGridSpec(
            num_scalar_prefetch=1,
            grid=(4,),
            in_specs=[
                whole_spec((2 * GROUP, REDUCED)),
                columns(2 * GROUP),
                columns(2 * GROUP),
                columns(128),
                pl.BlockSpec((REDUCED, BLOCK), lambda j, place: (0, place[j])),
                *[whole_spec((REDUCED, BLOCK))] * 4,
                *[whole_spec((CHUNK, REDUCED))] * 8,
            ],
            out_specs=pl.BlockSpec((64, 2, 8, BLOCK), lambda j, place: (0, 0, 0, place[j])),
            scratch_shapes=[pltpu.VMEM((2 * GROUP, BLOCK), bf16)],
        ),
        out_shape=jax.ShapeDtypeStruct((64, 2, 8, COLS), bf16),
        compiler_params=pltpu.CompilerParams(
            dimension_semantics=("arbitrary",), vmem_limit_bytes=LIMIT
        ),
        cost_estimate=pl.CostEstimate(
            flops=12 * GROUP * REDUCED * COLS, bytes_accessed=4 * REDUCED * COLS, transcendentals=0
        ),
    )(place, rows, *prepared, own, *other, *misfits)


def total_kernel(pieces, out):
    for u in range(2):
        total = pieces[0, u].astype(f32)
        for k in range(1, 16):
            total = total + pieces[k, u].astype(f32)
        out[0, :, u * COLS : (u + 1) * COLS] = total


def total_of(pieces):
    return pl.pallas_call(
        total_kernel,
        grid=(4,),
        in_specs=[pl.BlockSpec((16, 2, 8, COLS), lambda i: (0, i, 0, 0))],
        out_specs=pl.BlockSpec((1, 8, 2 * COLS), lambda i: (0, 0, i)),
        out_shape=jax.ShapeDtypeStruct((1, 8, 8 * COLS), f32),
        compiler_params=pltpu.CompilerParams(
            dimension_semantics=("arbitrary",), vmem_limit_bytes=LIMIT
        ),
    )(pieces)


def rows_at(array, order, places):
    picked = [lax.dynamic_slice_in_dim(array, order[k], 1, 0) for k in places]
    return jnp.concatenate(picked, axis=0)


def shards(samples, targets, jacobian_targets, directions, plan, weights):
    at_x, at_y = lax.axis_index("x"), lax.axis_index("y")
    zl, core, zh = lax.axis_index("zl"), lax.axis_index("core"), lax.axis_index("zh")
    z = zh * 2 + zl
    kind = (at_x + 2 * at_y) % 4
    weight = weights[0]
    mine = (zl * 2 + core) * 2 + zh
    theirs = ((1 - zl) * 2 + core) * 2 + (1 - zh)
    turn = [(kind + k) % 4 for k in range(4)]
    place = jnp.stack(turn + [zh]).astype(jnp.int32)

    quarter = lax.dynamic_slice_in_dim(weight, theirs * COLS + kind * BLOCK, BLOCK, 1)
    direct = z_facing(quarter)
    own = lax.dynamic_slice_in_dim(weight, mine * COLS, COLS, 1)

    order = plan[0, :MICRO]
    inputs = rows_at(samples, order, range(MICRO)).astype(f32)
    chosen = rows_at(directions, order, range(MICRO)).astype(f32)
    packed = jnp.concatenate([inputs, chosen], axis=1)
    swapped = core_swap(packed)
    direct, packed, swapped = lax.optimization_barrier((direct, packed, swapped))
    other = [
        direct,
        ring_shift(direct, "x", 3),
        ring_shift(direct, "y", 3),
        ring_shift(direct, "x", 1),
    ]
    pair = jnp.concatenate([packed, swapped], axis=0)
    beside = lax.ppermute(pair, "zl", [(0, 1), (1, 0)])
    low = jnp.where(zl == 0, pair, beside).reshape(2, 2, 2, REDUCED + TANGENTS)
    high = jnp.where(zl == 0, beside, pair).reshape(2, 2, 2, REDUCED + TANGENTS)
    small = jnp.stack([low, high], axis=2).reshape(2, 4, 2, REDUCED + TANGENTS)
    small = lax.dynamic_slice_in_dim(jnp.concatenate([small, small], axis=1), z, 4, 1)
    small = small.reshape(8, 2, REDUCED + TANGENTS)
    chosen = small[:, :, REDUCED:].reshape(8, 2 * TANGENTS).astype(jnp.int32)
    onehot = (chosen[:, :, None] == jnp.arange(REDUCED, dtype=jnp.int32)).astype(bf16)
    inputs = jnp.pad(small[:, :, :REDUCED].astype(bf16), ((0, 0), (0, 14), (0, 0)))
    rows = jnp.concatenate([onehot, inputs], axis=1).reshape(2 * GROUP, REDUCED)

    own_order = lax.dynamic_slice_in_dim(order, zh * 2, 2)
    target_rows = rows_at(targets, own_order, range(2)).astype(f32)
    target_jac = rows_at(jacobian_targets, own_order, range(2)).reshape(2 * TANGENTS, REDUCED)
    wanted = jnp.concatenate(
        [target_jac.astype(f32), jnp.pad(target_rows, ((0, 14), (0, 0)))], axis=0
    )

    from_core = core_swap(forward(place, rows, own, other))
    from_core, wanted = lax.optimization_barrier((from_core, wanted))
    chunks = forward(place, rows, own, other, from_core)
    chunks, ready = lax.optimization_barrier((chunks, rows))
    got = [z_shift(chunks[d], d) for d in (2, 1, 3)]
    prepared = prepare(place, ready, own, other)
    got, prepared = lax.optimization_barrier((got, prepared))
    total = chunks[0]
    for g in got:
        total = total + g.astype(f32)
    scale = jnp.where(jnp.arange(CHUNK)[:, None] < 2 * TANGENTS, jacobian_weight, 1.0)
    misfit = (scale * (total - wanted)).astype(bf16)
    near = [misfit, None, None, None]
    for d in (2, 1, 3):
        near[d] = z_shift(misfit, 4 - d)
    misfits = near + [core_swap(m) for m in near]
    sent = backward(place, rows, prepared, own, other, misfits)
    pieces = lax.all_to_all(
        sent.reshape(128, 8, COLS), AXES, split_axis=0, concat_axis=0, tiled=True
    )
    return total_of(pieces.reshape(16, 8, 8, COLS))


def solution(mesh):
    torus = Mesh(mesh.devices.reshape(4, 4, 2, 2, 2), AXES)
    return jax.shard_map(
        shards,
        mesh=torus,
        in_specs=(
            P(DP, None),
            P(DP, None),
            P(DP, None, None),
            P(DP, None),
            P(DP, None),
            P("zh", None, None),
        ),
        out_specs=P("zh", DP, None),
        check_vma=False,
    )
```

```python
import jax
import jax.numpy as jnp
from jax import lax
from jax.experimental import pallas as pl
from jax.experimental.pallas import tpu as pltpu
from jax.sharding import Mesh
from jax.sharding import PartitionSpec as P

AXES = ("x", "y", "zl", "core", "zh")
DP = ("x", "y", "zl", "core")
Z = ("zl", "zh")
MICRO = 4
REDUCED = 512
COLS = 1024
BLOCK = 256
TANGENTS = 128
CHUNK = 2 * TANGENTS + 16
GROUP = 4 * CHUNK
STEP = 2 * CHUNK
LIMIT = 24 * 2**20
jacobian_weight = 32.0
f32 = jnp.float32
bf16 = jnp.bfloat16


def z_index(z):
    return (z % 2) * 2 + z // 2


def z_shift(block, d):
    return lax.ppermute(block, Z, [(z_index(z), z_index((z + d) % 4)) for z in range(4)])


def z_facing(block):
    return lax.ppermute(block, Z, [(t, 3 - t) for t in range(4)])


def ring_shift(block, axis, d):
    return lax.ppermute(block, axis, [(i, (i + d) % 4) for i in range(4)])


def core_swap(block):
    return lax.ppermute(block, "core", [(0, 1), (1, 0)])


def slopes(linear):
    squash = jax.nn.sigmoid(linear)
    first = squash * (1.0 + linear * (1.0 - squash))
    second = squash * (1.0 - squash) * (2.0 + linear * (1.0 - 2.0 * squash))
    return linear * squash, first, second


def per_row(top, first):
    return [top[:TANGENTS] * first[0:1], top[TANGENTS : 2 * TANGENTS] * first[1:2]]


def whole_spec(shape):
    return pl.BlockSpec(shape, lambda i, place: (0,) * len(shape))


def own_specs():
    return [pl.BlockSpec((REDUCED, BLOCK), lambda i, place, k=k: (0, place[k])) for k in range(4)]


def forward_kernel(final, place, rows, *refs):
    own, other, refs = refs[:4], refs[4:8], refs[8:]
    if final:
        arrived, refs = refs[0], refs[1:]
    w_first, w_last = refs[-2:]
    outs = refs[:-2]

    @pl.when(pl.program_id(0) == 0)
    def _():
        here = place[4] == 0
        for k in range(4):
            span = slice(k * BLOCK, (k + 1) * BLOCK)
            w_first[:, span] = jnp.where(here, own[k][...], other[k][...])
            w_last[:, span] = jnp.where(here, other[k][...], own[k][...])

    picked = jnp.dot(rows[...], w_first[...], preferred_element_type=f32)
    parts = []
    for c in range(2):
        part = picked[c * CHUNK : (c + 1) * CHUNK]
        hidden, first, _ = slopes(part[2 * TANGENTS :])
        parts += per_row(part, first) + [hidden]
    tangent = jnp.concatenate(parts, axis=0).astype(bf16)
    total = lax.dot_general(
        tangent, w_last[...], (((1,), (1,)), ((), ())), preferred_element_type=f32
    )
    if not final:
        outs[0][...] = total.astype(bf16)
        return
    total = total + arrived[...].astype(f32)
    for step in range(2):

        @pl.when(pl.program_id(0) == step)
        def _():
            for c in range(2):
                out = outs[2 * step + c]
                out[...] = total[c * CHUNK : (c + 1) * CHUNK].astype(out.dtype)


def forward(place, rows, own, other, arrived=None):
    final = arrived is not None
    base = 0 if final else 2
    in_specs = [pl.BlockSpec((STEP, REDUCED), lambda i, place: (i + base, 0)), *own_specs()]
    in_specs += [whole_spec((REDUCED, BLOCK))] * 4
    args = [rows, own, own, own, own, *other]
    out_specs = pl.BlockSpec((STEP, REDUCED), lambda i, place: (i, 0))
    out_shape = jax.ShapeDtypeStruct((GROUP, REDUCED), bf16)
    if final:
        in_specs.append(out_specs)
        args.append(arrived)
        out_specs = [whole_spec((CHUNK, REDUCED))] * 4
        out_shape = [jax.ShapeDtypeStruct((CHUNK, REDUCED), f32)]
        out_shape += [jax.ShapeDtypeStruct((CHUNK, REDUCED), bf16)] * 3
    return pl.pallas_call(
        lambda *refs: forward_kernel(final, *refs),
        grid_spec=pltpu.PrefetchScalarGridSpec(
            num_scalar_prefetch=1,
            grid=(2,),
            in_specs=in_specs,
            out_specs=out_specs,
            scratch_shapes=[pltpu.VMEM((REDUCED, COLS), bf16)] * 2,
        ),
        out_shape=out_shape,
        compiler_params=pltpu.CompilerParams(
            dimension_semantics=("arbitrary",), vmem_limit_bytes=LIMIT
        ),
        cost_estimate=pl.CostEstimate(
            flops=4 * GROUP * REDUCED * COLS, bytes_accessed=4 * REDUCED * COLS, transcendentals=0
        ),
    )(place, *args)


def piece_of(step, pieces):
    chosen = pieces[3][...]
    for k in range(3):
        chosen = jnp.where(step == k, pieces[k][...], chosen)
    return chosen


def prepare_kernel(place, rows, own, *refs):
    other, (picked_out, tangents, linears) = refs[:4], refs[4:]
    theirs = piece_of(pl.program_id(0), other)
    w_first = jnp.where(place[4] == 0, own[...], theirs)
    for c in range(0, 8, 2):
        span = pl.ds(c * CHUNK, STEP)
        picked = jnp.dot(rows[span, :], w_first, preferred_element_type=f32)
        picked_out[span, :] = picked.astype(bf16)
        parts = []
        for e in range(2):
            part = picked[e * CHUNK : (e + 1) * CHUNK]
            linear = part[2 * TANGENTS :]
            hidden, first, _ = slopes(linear)
            parts += per_row(part, first) + [hidden]
            linears[pl.ds((c + e) * 16, 16), :] = linear
        tangents[span, :] = jnp.concatenate(parts, axis=0).astype(bf16)


def prepare(place, rows, own, other):
    columns = lambda height: pl.BlockSpec((height, BLOCK), lambda j, place: (0, j))
    return pl.pallas_call(
        prepare_kernel,
        grid_spec=pltpu.PrefetchScalarGridSpec(
            num_scalar_prefetch=1,
            grid=(4,),
            in_specs=[
                whole_spec((2 * GROUP, REDUCED)),
                pl.BlockSpec((REDUCED, BLOCK), lambda j, place: (0, place[j])),
                *[whole_spec((REDUCED, BLOCK))] * 4,
            ],
            out_specs=[columns(2 * GROUP), columns(2 * GROUP), columns(128)],
        ),
        out_shape=[
            jax.ShapeDtypeStruct((2 * GROUP, COLS), bf16),
            jax.ShapeDtypeStruct((2 * GROUP, COLS), bf16),
            jax.ShapeDtypeStruct((128, COLS), f32),
        ],
        compiler_params=pltpu.CompilerParams(
            dimension_semantics=("arbitrary",), vmem_limit_bytes=LIMIT
        ),
        cost_estimate=pl.CostEstimate(
            flops=4 * GROUP * REDUCED * COLS, bytes_accessed=4 * REDUCED * COLS, transcendentals=0
        ),
    )(place, rows, own, *other)


def backward_kernel(place, rows, picked, tangents, linears, own, *refs):
    other, misfits, out, cotangents = refs[:4], refs[4:12], refs[12], refs[13]
    theirs = piece_of(pl.program_id(0), other)
    w_last = jnp.where(place[4] == 0, theirs, own[...])
    for c in range(8):
        span = pl.ds(c * CHUNK, CHUNK)
        back = jnp.dot(misfits[c][...], w_last, preferred_element_type=f32)
        back = back.astype(bf16).astype(f32)
        _, first, second = slopes(linears[pl.ds(c * 16, 16), :])
        joint = back[: 2 * TANGENTS] * picked[pl.ds(c * CHUNK, 2 * TANGENTS), :].astype(f32)
        projected = jnp.concatenate(
            [
                jnp.sum(joint[:TANGENTS], axis=0, keepdims=True),
                jnp.sum(joint[TANGENTS:], axis=0, keepdims=True),
                jnp.zeros((14, BLOCK), f32),
            ],
            axis=0,
        )
        before = back[2 * TANGENTS :] * first + second * projected
        cotangents[span, :] = jnp.concatenate(per_row(back, first) + [before], axis=0).astype(bf16)
    over_rows = (((0,), (0,)), ((), ()))
    whole = jnp.concatenate([m[...] for m in misfits], axis=0)
    last = lax.dot_general(whole, tangents[...], over_rows, preferred_element_type=f32)
    first = lax.dot_general(rows[...], cotangents[...], over_rows, preferred_element_type=f32)
    out[:, 0] = first.astype(bf16).reshape(64, 8, BLOCK)
    out[:, 1] = last.astype(bf16).reshape(64, 8, BLOCK)


def backward(place, rows, prepared, own, other, misfits):
    columns = lambda height: pl.BlockSpec((height, BLOCK), lambda j, place: (0, j))
    return pl.pallas_call(
        backward_kernel,
        grid_spec=pltpu.PrefetchScalarGridSpec(
            num_scalar_prefetch=1,
            grid=(4,),
            in_specs=[
                whole_spec((2 * GROUP, REDUCED)),
                columns(2 * GROUP),
                columns(2 * GROUP),
                columns(128),
                pl.BlockSpec((REDUCED, BLOCK), lambda j, place: (0, place[j])),
                *[whole_spec((REDUCED, BLOCK))] * 4,
                *[whole_spec((CHUNK, REDUCED))] * 8,
            ],
            out_specs=pl.BlockSpec((64, 2, 8, BLOCK), lambda j, place: (0, 0, 0, place[j])),
            scratch_shapes=[pltpu.VMEM((2 * GROUP, BLOCK), bf16)],
        ),
        out_shape=jax.ShapeDtypeStruct((64, 2, 8, COLS), bf16),
        compiler_params=pltpu.CompilerParams(
            dimension_semantics=("arbitrary",), vmem_limit_bytes=LIMIT
        ),
        cost_estimate=pl.CostEstimate(
            flops=12 * GROUP * REDUCED * COLS, bytes_accessed=4 * REDUCED * COLS, transcendentals=0
        ),
    )(place, rows, *prepared, own, *other, *misfits)


def total_kernel(pieces, out):
    for u in range(2):
        total = pieces[0, u].astype(f32)
        for k in range(1, 16):
            total = total + pieces[k, u].astype(f32)
        out[0, :, u * COLS : (u + 1) * COLS] = total


def total_of(pieces):
    return pl.pallas_call(
        total_kernel,
        grid=(4,),
        in_specs=[pl.BlockSpec((16, 2, 8, COLS), lambda i: (0, i, 0, 0))],
        out_specs=pl.BlockSpec((1, 8, 2 * COLS), lambda i: (0, 0, i)),
        out_shape=jax.ShapeDtypeStruct((1, 8, 8 * COLS), f32),
        compiler_params=pltpu.CompilerParams(
            dimension_semantics=("arbitrary",), vmem_limit_bytes=LIMIT
        ),
    )(pieces)


def pick_kernel(order, place, samples, directions, targets, target_jac, packed, wanted):
    def chosen(rows, at):
        total = jnp.zeros_like(rows[0:1])
        for j in range(8):
            total = jnp.where(order[at] == j, rows[j : j + 1], total)
        return total

    step = pl.program_id(0)

    @pl.when(step == 0)
    def _():
        inputs = samples[...].astype(f32)
        places = directions[...].astype(f32)
        packed[:, :REDUCED] = jnp.concatenate([chosen(inputs, k) for k in range(MICRO)], axis=0)
        packed[:, REDUCED:] = jnp.concatenate([chosen(places, k) for k in range(MICRO)], axis=0)
        outputs = targets[...].astype(f32)
        own = [chosen(outputs, place[4] * 2 + k) for k in range(2)]
        wanted[2 * TANGENTS :, :] = jnp.concatenate([*own, jnp.zeros((14, REDUCED), f32)], axis=0)

    wanted[pl.ds(pl.multiple_of(step * TANGENTS, TANGENTS), TANGENTS), :] = target_jac[0].astype(f32)


def pick(order, place, samples, directions, targets, jacobian_targets):
    whole = lambda shape: pl.BlockSpec(shape, lambda i, order, place: (0, 0))
    return pl.pallas_call(
        pick_kernel,
        grid_spec=pltpu.PrefetchScalarGridSpec(
            num_scalar_prefetch=2,
            grid=(2,),
            in_specs=[
                whole((8, REDUCED)),
                whole((8, TANGENTS)),
                whole((8, REDUCED)),
                pl.BlockSpec(
                    (1, TANGENTS, REDUCED),
                    lambda i, order, place: (order[place[4] * 2 + i], 0, 0),
                ),
            ],
            out_specs=[whole((MICRO, REDUCED + TANGENTS)), whole((CHUNK, REDUCED))],
        ),
        out_shape=[
            jax.ShapeDtypeStruct((MICRO, REDUCED + TANGENTS), f32),
            jax.ShapeDtypeStruct((CHUNK, REDUCED), f32),
        ],
        compiler_params=pltpu.CompilerParams(
            dimension_semantics=("arbitrary",), vmem_limit_bytes=LIMIT
        ),
    )(order, place, samples, directions, targets, jacobian_targets)


def shards(samples, targets, jacobian_targets, directions, plan, weights):
    at_x, at_y = lax.axis_index("x"), lax.axis_index("y")
    zl, core, zh = lax.axis_index("zl"), lax.axis_index("core"), lax.axis_index("zh")
    z = zh * 2 + zl
    kind = (at_x + 2 * at_y) % 4
    weight = weights[0]
    mine = (zl * 2 + core) * 2 + zh
    theirs = ((1 - zl) * 2 + core) * 2 + (1 - zh)
    turn = [(kind + k) % 4 for k in range(4)]
    place = jnp.stack(turn + [zh]).astype(jnp.int32)

    quarter = lax.dynamic_slice_in_dim(weight, theirs * COLS + kind * BLOCK, BLOCK, 1)
    direct = z_facing(quarter)
    own = lax.dynamic_slice_in_dim(weight, mine * COLS, COLS, 1)

    packed, wanted = pick(
        plan.reshape(8), place, samples, directions, targets, jacobian_targets
    )
    swapped = core_swap(packed)
    direct, packed, swapped = lax.optimization_barrier((direct, packed, swapped))
    other = [
        direct,
        ring_shift(direct, "x", 3),
        ring_shift(direct, "y", 3),
        ring_shift(direct, "x", 1),
    ]
    pair = jnp.concatenate([packed, swapped], axis=0)
    beside = lax.ppermute(pair, "zl", [(0, 1), (1, 0)])
    low = jnp.where(zl == 0, pair, beside).reshape(2, 2, 2, REDUCED + TANGENTS)
    high = jnp.where(zl == 0, beside, pair).reshape(2, 2, 2, REDUCED + TANGENTS)
    small = jnp.stack([low, high], axis=2).reshape(2, 4, 2, REDUCED + TANGENTS)
    small = lax.dynamic_slice_in_dim(jnp.concatenate([small, small], axis=1), z, 4, 1)
    small = small.reshape(8, 2, REDUCED + TANGENTS)
    chosen = small[:, :, REDUCED:].reshape(8, 2 * TANGENTS).astype(jnp.int32)
    onehot = (chosen[:, :, None] == jnp.arange(REDUCED, dtype=jnp.int32)).astype(bf16)
    inputs = jnp.pad(small[:, :, :REDUCED].astype(bf16), ((0, 0), (0, 14), (0, 0)))
    rows = jnp.concatenate([onehot, inputs], axis=1).reshape(2 * GROUP, REDUCED)

    from_core = core_swap(forward(place, rows, own, other))
    chunks = forward(place, rows, own, other, from_core)
    chunks, ready = lax.optimization_barrier((chunks, rows))
    got = [z_shift(chunks[d], d) for d in (2, 1, 3)]
    prepared = prepare(place, ready, own, other)
    got, prepared = lax.optimization_barrier((got, prepared))
    total = chunks[0]
    for g in got:
        total = total + g.astype(f32)
    scale = jnp.where(jnp.arange(CHUNK)[:, None] < 2 * TANGENTS, jacobian_weight, 1.0)
    misfit = (scale * (total - wanted)).astype(bf16)
    near = [misfit, None, None, None]
    for d in (2, 1, 3):
        near[d] = z_shift(misfit, 4 - d)
    misfits = near + [core_swap(m) for m in near]
    sent = backward(place, rows, prepared, own, other, misfits)
    pieces = lax.all_to_all(
        sent.reshape(128, 8, COLS), AXES, split_axis=0, concat_axis=0, tiled=True
    )
    return total_of(pieces.reshape(16, 8, 8, COLS))


def solution(mesh):
    torus = Mesh(mesh.devices.reshape(4, 4, 2, 2, 2), AXES)
    return jax.shard_map(
        shards,
        mesh=torus,
        in_specs=(
            P(DP, None),
            P(DP, None),
            P(DP, None, None),
            P(DP, None),
            P(DP, None),
            P("zh", None, None),
        ),
        out_specs=P("zh", DP, None),
        check_vma=False,
    )
```

```python
import jax
import jax.numpy as jnp
from jax import lax
from jax.experimental import pallas as pl
from jax.experimental.pallas import tpu as pltpu
from jax.sharding import Mesh
from jax.sharding import PartitionSpec as P

AXES = ("x", "y", "zl", "core", "zh")
DP = ("x", "y", "zl", "core")
Z = ("zl", "zh")
MICRO = 4
REDUCED = 512
COLS = 1024
BLOCK = 256
TANGENTS = 128
CHUNK = 2 * TANGENTS + 16
GROUP = 4 * CHUNK
STEP = 2 * CHUNK
LIMIT = 24 * 2**20
ORDER = (0, 1, 3, 2)
EARLY = 6
jacobian_weight = 32.0
f32 = jnp.float32
bf16 = jnp.bfloat16


def z_index(z):
    return (z % 2) * 2 + z // 2


def z_shift(block, d):
    return lax.ppermute(block, Z, [(z_index(z), z_index((z + d) % 4)) for z in range(4)])


def z_facing(block):
    return lax.ppermute(block, Z, [(t, 3 - t) for t in range(4)])


def ring_shift(block, axis, d):
    return lax.ppermute(block, axis, [(i, (i + d) % 4) for i in range(4)])


def core_swap(block):
    return lax.ppermute(block, "core", [(0, 1), (1, 0)])


def slopes(linear):
    squash = jax.nn.sigmoid(linear)
    first = squash * (1.0 + linear * (1.0 - squash))
    second = squash * (1.0 - squash) * (2.0 + linear * (1.0 - 2.0 * squash))
    return linear * squash, first, second


def per_row(top, first):
    return [top[:TANGENTS] * first[0:1], top[TANGENTS : 2 * TANGENTS] * first[1:2]]


def whole_spec(shape):
    return pl.BlockSpec(shape, lambda i, place: (0,) * len(shape))


def own_specs():
    return [pl.BlockSpec((REDUCED, BLOCK), lambda i, place, k=k: (0, place[k])) for k in range(4)]


def forward_kernel(final, place, one, two, *refs):
    own, other, refs = refs[:4], refs[4:8], refs[8:]
    if final:
        arrived, refs = refs[0], refs[1:]
    w_first, w_last = refs[-2:]
    outs = refs[:-2]
    here = place[4] == 0
    for k in range(4):
        span = slice(k * BLOCK, (k + 1) * BLOCK)
        w_first[:, span] = jnp.where(here, own[k][...], other[k][...])
        w_last[:, span] = jnp.where(here, other[k][...], own[k][...])
    rows = jnp.concatenate([one[...], two[...]], axis=0)
    picked = jnp.dot(rows, w_first[...], preferred_element_type=f32)
    parts = []
    for c in range(2):
        part = picked[c * CHUNK : (c + 1) * CHUNK]
        hidden, first, _ = slopes(part[2 * TANGENTS :])
        parts += per_row(part, first) + [hidden]
    tangent = jnp.concatenate(parts, axis=0).astype(bf16)
    total = lax.dot_general(
        tangent, w_last[...], (((1,), (1,)), ((), ())), preferred_element_type=f32
    )
    if not final:
        outs[0][...] = total.astype(bf16)
        return
    total = total + arrived[...].astype(f32)
    for c in range(2):
        outs[c][...] = total[c * CHUNK : (c + 1) * CHUNK].astype(outs[c].dtype)


def forward(place, rows, at, own, other, arrived=None, dtypes=None):
    final = arrived is not None
    in_specs = [pl.BlockSpec((CHUNK, REDUCED), lambda i, place, a=a: (a, 0)) for a in at]
    in_specs += own_specs() + [whole_spec((REDUCED, BLOCK))] * 4
    args = [rows, rows, own, own, own, own, *other]
    out_specs = whole_spec((STEP, REDUCED))
    out_shape = jax.ShapeDtypeStruct((STEP, REDUCED), bf16)
    if final:
        in_specs.append(out_specs)
        args.append(arrived)
        out_specs = [whole_spec((CHUNK, REDUCED))] * 2
        out_shape = [jax.ShapeDtypeStruct((CHUNK, REDUCED), dtype) for dtype in dtypes]
    return pl.pallas_call(
        lambda *refs: forward_kernel(final, *refs),
        grid_spec=pltpu.PrefetchScalarGridSpec(
            num_scalar_prefetch=1,
            grid=(1,),
            in_specs=in_specs,
            out_specs=out_specs,
            scratch_shapes=[pltpu.VMEM((REDUCED, COLS), bf16)] * 2,
        ),
        out_shape=out_shape,
        compiler_params=pltpu.CompilerParams(
            dimension_semantics=("arbitrary",), vmem_limit_bytes=LIMIT
        ),
        cost_estimate=pl.CostEstimate(
            flops=4 * STEP * REDUCED * COLS, bytes_accessed=4 * REDUCED * COLS, transcendentals=0
        ),
    )(place, *args)


def piece_of(step, pieces):
    chosen = pieces[3][...]
    for k in range(3):
        chosen = jnp.where(step == k, pieces[k][...], chosen)
    return chosen


def prepare_kernel(place, rows, own, *refs):
    other, (picked_out, tangents, linears) = refs[:4], refs[4:]
    theirs = piece_of(pl.program_id(0), other)
    w_first = jnp.where(place[4] == 0, own[...], theirs)
    for c in range(0, 8, 2):
        span = pl.ds(c * CHUNK, STEP)
        picked = jnp.dot(rows[span, :], w_first, preferred_element_type=f32)
        picked_out[span, :] = picked.astype(bf16)
        parts = []
        for e in range(2):
            part = picked[e * CHUNK : (e + 1) * CHUNK]
            linear = part[2 * TANGENTS :]
            hidden, first, _ = slopes(linear)
            parts += per_row(part, first) + [hidden]
            linears[pl.ds((c + e) * 16, 16), :] = linear
        tangents[span, :] = jnp.concatenate(parts, axis=0).astype(bf16)


def prepare(place, rows, own, other):
    columns = lambda height: pl.BlockSpec((height, BLOCK), lambda j, place: (0, j))
    return pl.pallas_call(
        prepare_kernel,
        grid_spec=pltpu.PrefetchScalarGridSpec(
            num_scalar_prefetch=1,
            grid=(4,),
            in_specs=[
                whole_spec((2 * GROUP, REDUCED)),
                pl.BlockSpec((REDUCED, BLOCK), lambda j, place: (0, place[j])),
                *[whole_spec((REDUCED, BLOCK))] * 4,
            ],
            out_specs=[columns(2 * GROUP), columns(2 * GROUP), columns(128)],
        ),
        out_shape=[
            jax.ShapeDtypeStruct((2 * GROUP, COLS), bf16),
            jax.ShapeDtypeStruct((2 * GROUP, COLS), bf16),
            jax.ShapeDtypeStruct((128, COLS), f32),
        ],
        compiler_params=pltpu.CompilerParams(
            dimension_semantics=("arbitrary",), vmem_limit_bytes=LIMIT
        ),
        cost_estimate=pl.CostEstimate(
            flops=4 * GROUP * REDUCED * COLS, bytes_accessed=4 * REDUCED * COLS, transcendentals=0
        ),
    )(place, rows, own, *other)


def backward_kernel(count, place, rows, picked, tangents, linears, own, *refs):
    other, misfits, refs = refs[:4], refs[4 : 4 + count], refs[4 + count :]
    cotangents = refs[-1]
    theirs = piece_of(pl.program_id(0), other)
    w_last = jnp.where(place[4] == 0, theirs, own[...])
    for c in range(count):
        span = pl.ds(c * CHUNK, CHUNK)
        back = jnp.dot(misfits[c][...], w_last, preferred_element_type=f32)
        back = back.astype(bf16).astype(f32)
        _, first, second = slopes(linears[pl.ds(c * 16, 16), :])
        joint = back[: 2 * TANGENTS] * picked[pl.ds(c * CHUNK, 2 * TANGENTS), :].astype(f32)
        projected = jnp.concatenate(
            [
                jnp.sum(joint[:TANGENTS], axis=0, keepdims=True),
                jnp.sum(joint[TANGENTS:], axis=0, keepdims=True),
                jnp.zeros((14, BLOCK), f32),
            ],
            axis=0,
        )
        before = back[2 * TANGENTS :] * first + second * projected
        cotangents[span, :] = jnp.concatenate(per_row(back, first) + [before], axis=0).astype(bf16)
    over_rows = (((0,), (0,)), ((), ()))
    whole = jnp.concatenate([m[...] for m in misfits], axis=0)
    last = lax.dot_general(whole, tangents[...], over_rows, preferred_element_type=f32)
    first = lax.dot_general(rows[...], cotangents[...], over_rows, preferred_element_type=f32)
    if count == EARLY:
        first_out, last_out = refs[:2]
        first_out[...] = first
        last_out[...] = last
        return
    first_so_far, last_so_far, out = refs[:3]
    first = first + first_so_far[...]
    last = last + last_so_far[...]
    out[:, 0] = first.astype(bf16).reshape(64, 8, BLOCK)
    out[:, 1] = last.astype(bf16).reshape(64, 8, BLOCK)


def backward(place, rows, prepared, own, other, misfits, so_far=None):
    count = len(misfits)
    height, block = count * CHUNK, 0 if so_far is None else 3
    columns = lambda height, at=0: pl.BlockSpec((height, BLOCK), lambda j, place: (at, j))
    in_specs = [
        pl.BlockSpec((height, REDUCED), lambda j, place: (block, 0)),
        columns(height, block),
        columns(height, block),
        columns(16 * count, block),
        pl.BlockSpec((REDUCED, BLOCK), lambda j, place: (0, place[j])),
        *[whole_spec((REDUCED, BLOCK))] * 4,
        *[whole_spec((CHUNK, REDUCED))] * count,
    ]
    args = [rows, *prepared, own, *other, *misfits]
    if so_far is None:
        out_specs = [columns(REDUCED)] * 2
        out_shape = [jax.ShapeDtypeStruct((REDUCED, COLS), f32)] * 2
    else:
        in_specs += [columns(REDUCED)] * 2
        args += so_far
        out_specs = pl.BlockSpec((64, 2, 8, BLOCK), lambda j, place: (0, 0, 0, place[j]))
        out_shape = jax.ShapeDtypeStruct((64, 2, 8, COLS), bf16)
    return pl.pallas_call(
        lambda *refs: backward_kernel(count, *refs),
        grid_spec=pltpu.PrefetchScalarGridSpec(
            num_scalar_prefetch=1,
            grid=(4,),
            in_specs=in_specs,
            out_specs=out_specs,
            scratch_shapes=[pltpu.VMEM((height, BLOCK), bf16)],
        ),
        out_shape=out_shape,
        compiler_params=pltpu.CompilerParams(
            dimension_semantics=("arbitrary",), vmem_limit_bytes=LIMIT
        ),
        cost_estimate=pl.CostEstimate(
            flops=6 * height * REDUCED * COLS, bytes_accessed=4 * REDUCED * COLS, transcendentals=0
        ),
    )(place, *args)


def total_kernel(pieces, out):
    for u in range(2):
        total = pieces[0, u].astype(f32)
        for k in range(1, 16):
            total = total + pieces[k, u].astype(f32)
        out[0, :, u * COLS : (u + 1) * COLS] = total


def total_of(pieces):
    return pl.pallas_call(
        total_kernel,
        grid=(4,),
        in_specs=[pl.BlockSpec((16, 2, 8, COLS), lambda i: (0, i, 0, 0))],
        out_specs=pl.BlockSpec((1, 8, 2 * COLS), lambda i: (0, 0, i)),
        out_shape=jax.ShapeDtypeStruct((1, 8, 8 * COLS), f32),
        compiler_params=pltpu.CompilerParams(
            dimension_semantics=("arbitrary",), vmem_limit_bytes=LIMIT
        ),
    )(pieces)


def pick_kernel(order, place, samples, directions, targets, target_jac, packed, wanted):
    def chosen(rows, at):
        total = jnp.zeros_like(rows[0:1])
        for j in range(8):
            total = jnp.where(order[at] == j, rows[j : j + 1], total)
        return total

    step = pl.program_id(0)

    @pl.when(step == 0)
    def _():
        inputs = samples[...].astype(f32)
        places = directions[...].astype(f32)
        packed[:, :REDUCED] = jnp.concatenate([chosen(inputs, k) for k in range(MICRO)], axis=0)
        packed[:, REDUCED:] = jnp.concatenate([chosen(places, k) for k in range(MICRO)], axis=0)
        outputs = targets[...].astype(f32)
        own = [chosen(outputs, place[4] * 2 + k) for k in range(2)]
        wanted[2 * TANGENTS :, :] = jnp.concatenate([*own, jnp.zeros((14, REDUCED), f32)], axis=0)

    wanted[pl.ds(pl.multiple_of(step * TANGENTS, TANGENTS), TANGENTS), :] = target_jac[0].astype(f32)


def pick(order, place, samples, directions, targets, jacobian_targets):
    whole = lambda shape: pl.BlockSpec(shape, lambda i, order, place: (0, 0))
    return pl.pallas_call(
        pick_kernel,
        grid_spec=pltpu.PrefetchScalarGridSpec(
            num_scalar_prefetch=2,
            grid=(2,),
            in_specs=[
                whole((8, REDUCED)),
                whole((8, TANGENTS)),
                whole((8, REDUCED)),
                pl.BlockSpec(
                    (1, TANGENTS, REDUCED),
                    lambda i, order, place: (order[place[4] * 2 + i], 0, 0),
                ),
            ],
            out_specs=[whole((MICRO, REDUCED + TANGENTS)), whole((CHUNK, REDUCED))],
        ),
        out_shape=[
            jax.ShapeDtypeStruct((MICRO, REDUCED + TANGENTS), f32),
            jax.ShapeDtypeStruct((CHUNK, REDUCED), f32),
        ],
        compiler_params=pltpu.CompilerParams(
            dimension_semantics=("arbitrary",), vmem_limit_bytes=LIMIT
        ),
    )(order, place, samples, directions, targets, jacobian_targets)


def shards(samples, targets, jacobian_targets, directions, plan, weights):
    at_x, at_y = lax.axis_index("x"), lax.axis_index("y")
    zl, core, zh = lax.axis_index("zl"), lax.axis_index("core"), lax.axis_index("zh")
    z = zh * 2 + zl
    kind = (at_x + 2 * at_y) % 4
    weight = weights[0]
    share = (zl * 2 + core) * 2 + zh
    theirs = ((1 - zl) * 2 + core) * 2 + (1 - zh)
    turn = [(kind + k) % 4 for k in range(4)]
    place = jnp.stack(turn + [zh]).astype(jnp.int32)

    quarter = lax.dynamic_slice_in_dim(weight, theirs * COLS + kind * BLOCK, BLOCK, 1)
    direct = z_facing(quarter)
    own = lax.dynamic_slice_in_dim(weight, share * COLS, COLS, 1)

    packed, wanted = pick(
        plan.reshape(8), place, samples, directions, targets, jacobian_targets
    )
    swapped = core_swap(packed)
    direct, packed, swapped, own = lax.optimization_barrier((direct, packed, swapped, own))
    other = [
        direct,
        ring_shift(direct, "x", 3),
        ring_shift(direct, "y", 3),
        ring_shift(direct, "x", 1),
    ]
    pair = jnp.concatenate([packed, swapped], axis=0)
    beside = lax.ppermute(pair, "zl", [(0, 1), (1, 0)])
    low = jnp.where(zl == 0, pair, beside).reshape(2, 2, 2, REDUCED + TANGENTS)
    high = jnp.where(zl == 0, beside, pair).reshape(2, 2, 2, REDUCED + TANGENTS)
    small = jnp.stack([low, high], axis=2).reshape(2, 4, 2, REDUCED + TANGENTS)
    small = lax.dynamic_slice_in_dim(jnp.concatenate([small, small], axis=1), z, 4, 1)
    small = jnp.concatenate([small[:, d : d + 1] for d in ORDER], axis=1).swapaxes(0, 1)
    small = small.reshape(8, 2, REDUCED + TANGENTS)
    chosen = small[:, :, REDUCED:].reshape(8, 2 * TANGENTS).astype(jnp.int32)
    onehot = (chosen[:, :, None] == jnp.arange(REDUCED, dtype=jnp.int32)).astype(bf16)
    inputs = jnp.pad(small[:, :, :REDUCED].astype(bf16), ((0, 0), (0, 14), (0, 0)))
    rows = jnp.concatenate([onehot, inputs], axis=1).reshape(2 * GROUP, REDUCED)

    pairs = ((6, 2), (4, 0))
    arrived = []
    for one, two in pairs:
        arrived.append(core_swap(forward(place, rows, (one + 1, two + 1), own, other)))
    ahead = forward(place, rows, pairs[0], own, other, arrived[0], (bf16, bf16))
    ahead, second = lax.optimization_barrier((ahead, arrived[1]))
    got = [z_shift(ahead[0], 2), z_shift(ahead[1], 1)]
    three, total = forward(place, rows, pairs[1], own, other, second, (bf16, f32))
    got.append(z_shift(three, 3))
    total, ready = lax.optimization_barrier((total, rows))
    prepared = prepare(place, ready, own, other)
    got, prepared = lax.optimization_barrier((got, prepared))
    for g in got:
        total = total + g.astype(f32)
    scale = jnp.where(jnp.arange(CHUNK)[:, None] < 2 * TANGENTS, jacobian_weight, 1.0)
    misfit = (scale * (total - wanted)).astype(bf16)
    near, early = [misfit], []
    for d in ORDER[1:]:
        near.append(z_shift(misfit, 4 - d))
    for part in near[:3]:
        early += [part, core_swap(part)]
    so_far = backward(place, rows, prepared, own, other, early)
    near[3], so_far = lax.optimization_barrier((near[3], so_far))
    late = [near[3], core_swap(near[3])]
    sent = backward(place, rows, prepared, own, other, late, so_far)
    pieces = lax.all_to_all(
        sent.reshape(128, 8, COLS), AXES, split_axis=0, concat_axis=0, tiled=True
    )
    return total_of(pieces.reshape(16, 8, 8, COLS))


def solution(mesh):
    torus = Mesh(mesh.devices.reshape(4, 4, 2, 2, 2), AXES)
    return jax.shard_map(
        shards,
        mesh=torus,
        in_specs=(
            P(DP, None),
            P(DP, None),
            P(DP, None, None),
            P(DP, None),
            P(DP, None),
            P("zh", None, None),
        ),
        out_specs=P("zh", DP, None),
        check_vma=False,
    )
```

```python
import jax
import jax.numpy as jnp
from jax import lax
from jax.experimental import pallas as pl
from jax.experimental.pallas import tpu as pltpu
from jax.sharding import Mesh
from jax.sharding import PartitionSpec as P

AXES = ("x", "y", "zl", "core", "zh")
DP = ("x", "y", "zl", "core")
Z = ("zl", "zh")
MICRO = 4
REDUCED = 512
COLS = 1024
BLOCK = 256
TANGENTS = 128
CHUNK = 2 * TANGENTS + 16
GROUP = 4 * CHUNK
STEP = 2 * CHUNK
LIMIT = 24 * 2**20
PLACES = (0, 4, 1, 3, 5, 7, 2, 6)
EARLY = 4
jacobian_weight = 32.0
f32 = jnp.float32
bf16 = jnp.bfloat16


def z_index(z):
    return (z % 2) * 2 + z // 2


def z_shift(block, d):
    return lax.ppermute(block, Z, [(z_index(z), z_index((z + d) % 4)) for z in range(4)])


def z_facing(block):
    return lax.ppermute(block, Z, [(t, 3 - t) for t in range(4)])


def ring_shift(block, axis, d):
    return lax.ppermute(block, axis, [(i, (i + d) % 4) for i in range(4)])


def core_swap(block):
    return lax.ppermute(block, "core", [(0, 1), (1, 0)])


def slopes(linear):
    squash = jax.nn.sigmoid(linear)
    first = squash * (1.0 + linear * (1.0 - squash))
    second = squash * (1.0 - squash) * (2.0 + linear * (1.0 - 2.0 * squash))
    return linear * squash, first, second


def per_row(top, first):
    return [top[:TANGENTS] * first[0:1], top[TANGENTS : 2 * TANGENTS] * first[1:2]]


def whole_spec(shape):
    return pl.BlockSpec(shape, lambda i, place: (0,) * len(shape))


def own_specs():
    return [pl.BlockSpec((REDUCED, BLOCK), lambda i, place, k=k: (0, place[k])) for k in range(4)]


def forward_kernel(final, place, one, two, *refs):
    own, other, refs = refs[:4], refs[4:8], refs[8:]
    if final:
        arrived, refs = refs[0], refs[1:]
    w_first, w_last = refs[-2:]
    outs = refs[:-2]
    here = place[4] == 0
    for k in range(4):
        span = slice(k * BLOCK, (k + 1) * BLOCK)
        w_first[:, span] = jnp.where(here, own[k][...], other[k][...])
        w_last[:, span] = jnp.where(here, other[k][...], own[k][...])
    rows = jnp.concatenate([one[...], two[...]], axis=0)
    picked = jnp.dot(rows, w_first[...], preferred_element_type=f32)
    parts = []
    for c in range(2):
        part = picked[c * CHUNK : (c + 1) * CHUNK]
        hidden, first, _ = slopes(part[2 * TANGENTS :])
        parts += per_row(part, first) + [hidden]
    tangent = jnp.concatenate(parts, axis=0).astype(bf16)
    total = lax.dot_general(
        tangent, w_last[...], (((1,), (1,)), ((), ())), preferred_element_type=f32
    )
    if not final:
        outs[0][...] = total.astype(bf16)
        return
    total = total + arrived[...].astype(f32)
    for c in range(2):
        outs[c][...] = total[c * CHUNK : (c + 1) * CHUNK].astype(outs[c].dtype)


def forward(place, rows, at, own, other, arrived=None, dtypes=None):
    final = arrived is not None
    in_specs = [pl.BlockSpec((CHUNK, REDUCED), lambda i, place, a=a: (a, 0)) for a in at]
    in_specs += own_specs() + [whole_spec((REDUCED, BLOCK))] * 4
    args = [rows, rows, own, own, own, own, *other]
    out_specs = whole_spec((STEP, REDUCED))
    out_shape = jax.ShapeDtypeStruct((STEP, REDUCED), bf16)
    if final:
        in_specs.append(out_specs)
        args.append(arrived)
        out_specs = [whole_spec((CHUNK, REDUCED))] * 2
        out_shape = [jax.ShapeDtypeStruct((CHUNK, REDUCED), dtype) for dtype in dtypes]
    return pl.pallas_call(
        lambda *refs: forward_kernel(final, *refs),
        grid_spec=pltpu.PrefetchScalarGridSpec(
            num_scalar_prefetch=1,
            grid=(1,),
            in_specs=in_specs,
            out_specs=out_specs,
            scratch_shapes=[pltpu.VMEM((REDUCED, COLS), bf16)] * 2,
        ),
        out_shape=out_shape,
        compiler_params=pltpu.CompilerParams(
            dimension_semantics=("arbitrary",), vmem_limit_bytes=LIMIT
        ),
        cost_estimate=pl.CostEstimate(
            flops=4 * STEP * REDUCED * COLS, bytes_accessed=4 * REDUCED * COLS, transcendentals=0
        ),
    )(place, *args)


def piece_of(step, pieces):
    chosen = pieces[3][...]
    for k in range(3):
        chosen = jnp.where(step == k, pieces[k][...], chosen)
    return chosen


def prepare_kernel(place, rows, own, *refs):
    other, (picked_out, tangents, linears) = refs[:4], refs[4:]
    theirs = piece_of(pl.program_id(0), other)
    w_first = jnp.where(place[4] == 0, own[...], theirs)
    for c in range(0, 8, 2):
        span = pl.ds(c * CHUNK, STEP)
        picked = jnp.dot(rows[span, :], w_first, preferred_element_type=f32)
        picked_out[span, :] = picked.astype(bf16)
        parts = []
        for e in range(2):
            part = picked[e * CHUNK : (e + 1) * CHUNK]
            linear = part[2 * TANGENTS :]
            hidden, first, _ = slopes(linear)
            parts += per_row(part, first) + [hidden]
            linears[pl.ds((c + e) * 16, 16), :] = linear
        tangents[span, :] = jnp.concatenate(parts, axis=0).astype(bf16)


def prepare(place, rows, own, other):
    columns = lambda height: pl.BlockSpec((height, BLOCK), lambda j, place: (0, j))
    return pl.pallas_call(
        prepare_kernel,
        grid_spec=pltpu.PrefetchScalarGridSpec(
            num_scalar_prefetch=1,
            grid=(4,),
            in_specs=[
                whole_spec((2 * GROUP, REDUCED)),
                pl.BlockSpec((REDUCED, BLOCK), lambda j, place: (0, place[j])),
                *[whole_spec((REDUCED, BLOCK))] * 4,
            ],
            out_specs=[columns(2 * GROUP), columns(2 * GROUP), columns(128)],
        ),
        out_shape=[
            jax.ShapeDtypeStruct((2 * GROUP, COLS), bf16),
            jax.ShapeDtypeStruct((2 * GROUP, COLS), bf16),
            jax.ShapeDtypeStruct((128, COLS), f32),
        ],
        compiler_params=pltpu.CompilerParams(
            dimension_semantics=("arbitrary",), vmem_limit_bytes=LIMIT
        ),
        cost_estimate=pl.CostEstimate(
            flops=4 * GROUP * REDUCED * COLS, bytes_accessed=4 * REDUCED * COLS, transcendentals=0
        ),
    )(place, rows, own, *other)


def backward_kernel(count, place, rows, picked, tangents, linears, *refs):
    own, other, misfits, refs = refs[:4], refs[4:8], refs[8 : 8 + count], refs[8 + count :]
    w_last, cotangents = refs[-2:]
    outs = refs[:-2]
    here = place[4] == 0
    for k in range(4):
        w_last[:, k * BLOCK : (k + 1) * BLOCK] = jnp.where(here, other[k][...], own[k][...])
    whole = jnp.concatenate([m[...] for m in misfits], axis=0)
    for c in range(0, count, 2):
        back = jnp.dot(
            whole[c * CHUNK : (c + 2) * CHUNK], w_last[...], preferred_element_type=f32
        )
        parts = []
        for e in range(2):
            part = back[e * CHUNK : (e + 1) * CHUNK].astype(bf16).astype(f32)
            _, first, second = slopes(linears[(c + e) * 16 : (c + e + 1) * 16, :])
            start = (c + e) * CHUNK
            joint = part[: 2 * TANGENTS] * picked[start : start + 2 * TANGENTS, :].astype(f32)
            projected = jnp.concatenate(
                [
                    jnp.sum(joint[:TANGENTS], axis=0, keepdims=True),
                    jnp.sum(joint[TANGENTS:], axis=0, keepdims=True),
                    jnp.zeros((14, COLS), f32),
                ],
                axis=0,
            )
            before = part[2 * TANGENTS :] * first + second * projected
            parts += per_row(part, first) + [before]
        cotangents[c * CHUNK : (c + 2) * CHUNK, :] = jnp.concatenate(parts, axis=0).astype(bf16)
    over_rows = (((0,), (0,)), ((), ()))
    last = lax.dot_general(whole, tangents[...], over_rows, preferred_element_type=f32)
    first = lax.dot_general(rows[...], cotangents[...], over_rows, preferred_element_type=f32)
    if len(outs) == 2:
        outs[0][...] = first
        outs[1][...] = last
        return
    first_so_far, last_so_far, out = outs
    out[:, 0] = (first + first_so_far[...]).astype(bf16).reshape(64, 8, COLS)
    out[:, 1] = (last + last_so_far[...]).astype(bf16).reshape(64, 8, COLS)


def backward(place, rows, prepared, own, other, misfits, so_far=None):
    count = len(misfits)
    height, block = count * CHUNK, 0 if so_far is None else 1
    columns = lambda height, at=0: pl.BlockSpec((height, COLS), lambda j, place: (at, 0))
    in_specs = [
        pl.BlockSpec((height, REDUCED), lambda j, place: (block, 0)),
        columns(height, block),
        columns(height, block),
        columns(16 * count, block),
        *own_specs(),
        *[whole_spec((REDUCED, BLOCK))] * 4,
        *[whole_spec((CHUNK, REDUCED))] * count,
    ]
    args = [rows, *prepared, own, own, own, own, *other, *misfits]
    if so_far is None:
        out_specs = [columns(REDUCED)] * 2
        out_shape = [jax.ShapeDtypeStruct((REDUCED, COLS), f32)] * 2
    else:
        in_specs += [columns(REDUCED)] * 2
        args += so_far
        out_specs = whole_spec((64, 2, 8, COLS))
        out_shape = jax.ShapeDtypeStruct((64, 2, 8, COLS), bf16)
    return pl.pallas_call(
        lambda *refs: backward_kernel(count, *refs),
        grid_spec=pltpu.PrefetchScalarGridSpec(
            num_scalar_prefetch=1,
            grid=(1,),
            in_specs=in_specs,
            out_specs=out_specs,
            scratch_shapes=[
                pltpu.VMEM((REDUCED, COLS), bf16),
                pltpu.VMEM((height, COLS), bf16),
            ],
        ),
        out_shape=out_shape,
        compiler_params=pltpu.CompilerParams(
            dimension_semantics=("arbitrary",), vmem_limit_bytes=LIMIT
        ),
        cost_estimate=pl.CostEstimate(
            flops=6 * height * REDUCED * COLS, bytes_accessed=4 * REDUCED * COLS, transcendentals=0
        ),
    )(place, *args)


def total_kernel(pieces, out):
    for u in range(2):
        for block in range(4):
            total = jnp.zeros((8, BLOCK), f32)
            for k in range(16):
                at = (block - (k // 4 + 2 * (k % 4))) % 4 * BLOCK
                total = total + pieces[k, u, :, at : at + BLOCK].astype(f32)
            start = u * COLS + block * BLOCK
            out[0, :, start : start + BLOCK] = total


def total_of(pieces):
    return pl.pallas_call(
        total_kernel,
        grid=(4,),
        in_specs=[pl.BlockSpec((16, 2, 8, COLS), lambda i: (0, i, 0, 0))],
        out_specs=pl.BlockSpec((1, 8, 2 * COLS), lambda i: (0, 0, i)),
        out_shape=jax.ShapeDtypeStruct((1, 8, 8 * COLS), f32),
        compiler_params=pltpu.CompilerParams(
            dimension_semantics=("arbitrary",), vmem_limit_bytes=LIMIT
        ),
    )(pieces)


def pick_kernel(order, place, samples, directions, targets, target_jac, packed, wanted):
    def chosen(rows, at):
        total = jnp.zeros_like(rows[0:1])
        for j in range(8):
            total = jnp.where(order[at] == j, rows[j : j + 1], total)
        return total

    step = pl.program_id(0)

    @pl.when(step == 0)
    def _():
        inputs = samples[...].astype(f32)
        places = directions[...].astype(f32)
        packed[:, :REDUCED] = jnp.concatenate([chosen(inputs, k) for k in range(MICRO)], axis=0)
        packed[:, REDUCED:] = jnp.concatenate([chosen(places, k) for k in range(MICRO)], axis=0)
        outputs = targets[...].astype(f32)
        own = [chosen(outputs, place[4] * 2 + k) for k in range(2)]
        wanted[2 * TANGENTS :, :] = jnp.concatenate([*own, jnp.zeros((14, REDUCED), f32)], axis=0)

    wanted[pl.ds(pl.multiple_of(step * TANGENTS, TANGENTS), TANGENTS), :] = target_jac[0].astype(f32)


def pick(order, place, samples, directions, targets, jacobian_targets):
    whole = lambda shape: pl.BlockSpec(shape, lambda i, order, place: (0, 0))
    return pl.pallas_call(
        pick_kernel,
        grid_spec=pltpu.PrefetchScalarGridSpec(
            num_scalar_prefetch=2,
            grid=(2,),
            in_specs=[
                whole((8, REDUCED)),
                whole((8, TANGENTS)),
                whole((8, REDUCED)),
                pl.BlockSpec(
                    (1, TANGENTS, REDUCED),
                    lambda i, order, place: (order[place[4] * 2 + i], 0, 0),
                ),
            ],
            out_specs=[whole((MICRO, REDUCED + TANGENTS)), whole((CHUNK, REDUCED))],
        ),
        out_shape=[
            jax.ShapeDtypeStruct((MICRO, REDUCED + TANGENTS), f32),
            jax.ShapeDtypeStruct((CHUNK, REDUCED), f32),
        ],
        compiler_params=pltpu.CompilerParams(
            dimension_semantics=("arbitrary",), vmem_limit_bytes=LIMIT
        ),
    )(order, place, samples, directions, targets, jacobian_targets)


def shards(samples, targets, jacobian_targets, directions, plan, weights):
    at_x, at_y = lax.axis_index("x"), lax.axis_index("y")
    zl, core, zh = lax.axis_index("zl"), lax.axis_index("core"), lax.axis_index("zh")
    z = zh * 2 + zl
    kind = (at_x + 2 * at_y) % 4
    weight = weights[0]
    share = (zl * 2 + core) * 2 + zh
    theirs = ((1 - zl) * 2 + core) * 2 + (1 - zh)
    turn = [(kind + k) % 4 for k in range(4)]
    place = jnp.stack(turn + [zh]).astype(jnp.int32)

    quarter = lax.dynamic_slice_in_dim(weight, theirs * COLS + kind * BLOCK, BLOCK, 1)
    direct = z_facing(quarter)
    own = lax.dynamic_slice_in_dim(weight, share * COLS, COLS, 1)

    packed, wanted = pick(
        plan.reshape(8), place, samples, directions, targets, jacobian_targets
    )
    swapped = core_swap(packed)
    direct, packed, swapped, own = lax.optimization_barrier((direct, packed, swapped, own))
    other = [
        direct,
        ring_shift(direct, "x", 3),
        ring_shift(direct, "y", 3),
        ring_shift(direct, "x", 1),
    ]
    pair = jnp.concatenate([packed, swapped], axis=0)
    beside = lax.ppermute(pair, "zl", [(0, 1), (1, 0)])
    low = jnp.where(zl == 0, pair, beside).reshape(2, 2, 2, REDUCED + TANGENTS)
    high = jnp.where(zl == 0, beside, pair).reshape(2, 2, 2, REDUCED + TANGENTS)
    small = jnp.stack([low, high], axis=2).reshape(2, 4, 2, REDUCED + TANGENTS)
    small = lax.dynamic_slice_in_dim(jnp.concatenate([small, small], axis=1), z, 4, 1)
    small = small.reshape(8, 2, REDUCED + TANGENTS)
    small = jnp.concatenate([small[p : p + 1] for p in PLACES], axis=0)
    chosen = small[:, :, REDUCED:].reshape(8, 2 * TANGENTS).astype(jnp.int32)
    onehot = (chosen[:, :, None] == jnp.arange(REDUCED, dtype=jnp.int32)).astype(bf16)
    inputs = jnp.pad(small[:, :, :REDUCED].astype(bf16), ((0, 0), (0, 14), (0, 0)))
    rows = jnp.concatenate([onehot, inputs], axis=1).reshape(2 * GROUP, REDUCED)

    at = PLACES.index
    pairs = ((2, 1), (3, 0))
    arrived = []
    for one, two in pairs:
        arrived.append(core_swap(forward(place, rows, (at(4 + one), at(4 + two)), own, other)))
    pairs = [(at(one), at(two)) for one, two in pairs]
    ahead = forward(place, rows, pairs[0], own, other, arrived[0], (bf16, bf16))
    ahead, second = lax.optimization_barrier((ahead, arrived[1]))
    got = [z_shift(ahead[0], 2), z_shift(ahead[1], 1)]
    three, total = forward(place, rows, pairs[1], own, other, second, (bf16, f32))
    got.append(z_shift(three, 3))
    total, ready = lax.optimization_barrier((total, rows))
    prepared = prepare(place, ready, own, other)
    got, prepared = lax.optimization_barrier((got, prepared))
    for g in got:
        total = total + g.astype(f32)
    scale = jnp.where(jnp.arange(CHUNK)[:, None] < 2 * TANGENTS, jacobian_weight, 1.0)
    misfit = (scale * (total - wanted)).astype(bf16)
    parts = {0: misfit}
    for d in (1, 3, 2):
        parts[d] = z_shift(misfit, 4 - d)
    for d in (0, 1, 3):
        parts[4 + d] = core_swap(parts[d])
    so_far = backward(place, rows, prepared, own, other, [parts[p] for p in PLACES[:EARLY]])
    parts[2], so_far = lax.optimization_barrier((parts[2], so_far))
    parts[6] = core_swap(parts[2])
    late = [parts[p] for p in PLACES[EARLY:]]
    sent = backward(place, rows, prepared, own, other, late, so_far)
    pieces = lax.all_to_all(
        sent.reshape(128, 8, COLS), AXES, split_axis=0, concat_axis=0, tiled=True
    )
    return total_of(pieces.reshape(16, 8, 8, COLS))


def solution(mesh):
    torus = Mesh(mesh.devices.reshape(4, 4, 2, 2, 2), AXES)
    return jax.shard_map(
        shards,
        mesh=torus,
        in_specs=(
            P(DP, None),
            P(DP, None),
            P(DP, None, None),
            P(DP, None),
            P(DP, None),
            P("zh", None, None),
        ),
        out_specs=P("zh", DP, None),
        check_vma=False,
    )
```
